256 devices in a mesh: il: 2 (over core), xl: 4 (over x), ta: 32 (over z, y).
Axes of the slice: x: 4, y: 4, z: 8, core: 2. Of those that a mesh axis runs over, the one named last changes fastest.
Arguments:
- traces: float32 [32, 832, 8192], P('il', 'xl', 'ta'), may hold values from -6 to 6
- bin_steps: int32 [2, 32, 832], P(None, 'il', 'xl'), may hold values from -1 to 1
Outputs:
- regridded: float32 [16, 416, 12288], P('il', 'xl', 'ta')
The draws below stay inside these ranges and needn't reach their ends.
Inputs may be any that keep to these rules, and one draw needn't show every extreme that they name: `bin_steps`: every entry is -1, 0 or 1.
All inputs are finite; a program needn't handle non-finite values.
Results may differ from the reference program's by a relative error of at most 0.0001.
Values sent between devices are 32-bit elements; how exact they have to be, the bound alone decides.
A program may use at most 128 MiB of HBM per device.

```python
import jax
import jax.numpy as jnp
from jax import lax

CT = 256
TAPS = 16
P_SIZE = 3
Q = 2
NI = 32
NX = 832
NT = 8192
BI = 16
BX = 416
N_TA = 32


def set_ends(entries, own_key, low, largest):
    longest = entries.shape.index(max(entries.shape))
    spots = []
    for shift in (0, 1):
        where = [jax.random.randint(jax.random.fold_in(own_key, axis), (), 0, length) for axis, length in enumerate(entries.shape)]
        where[longest] = (where[longest] + shift) % entries.shape[longest]
        spots.append(tuple(where))
    return entries.at[spots[0]].set(low).at[spots[1]].set(largest)


def block_scale(key, shape, cuts, smallest, high):
    loudness, own = 1.0, jax.random.fold_in(key, 6)
    for dim, blocks in cuts:
        draws = jnp.exp(jax.random.uniform(jax.random.fold_in(own, dim), (blocks,), jnp.float32, smallest / len(cuts), high / len(cuts)))
        loudness = loudness * jnp.repeat(draws, shape[dim] // blocks).reshape([-1 if axis == dim else 1 for axis in range(len(shape))])
    return loudness


def gaussian(key, dims, spread, most, split=(), kind=jnp.bfloat16):
    drawn = spread * jax.random.normal(key, dims, jnp.float32)
    if split:
        drawn = drawn * block_scale(key, dims, split, -0.22, 0.18)
    return jnp.clip(drawn, -most, most).astype(kind)


def setup_inputs(seed: int = 0) -> dict:
    streams_of = jax.random.split(jax.random.key(seed), 3)
    traces = gaussian(streams_of[0], (NI, NX, NT), 1.0, 6.0, ((0, 2), (1, 4), (2, 32)), jnp.float32)
    bin_steps = set_ends(jax.random.randint(streams_of[1], (2, NI, NX), -1, 2), jax.random.fold_in(streams_of[1], 1), -1, 1).astype(jnp.int32)
    return {"traces": traces, "bin_steps": bin_steps}


def lanczos_table(row_count, col_count, tap_reach, ratio_p, ratio_q):
    row_ids = lax.broadcasted_iota(jnp.int32, (row_count, col_count), 0)
    col_ids = lax.broadcasted_iota(jnp.int32, (row_count, col_count), 1)
    offset = (col_ids * ratio_q - (row_ids - tap_reach) * ratio_p).astype(jnp.float32) / jnp.float32(ratio_p)
    inside = jnp.abs(offset) < jnp.float32(tap_reach)
    weights = jnp.sinc(offset) * jnp.sinc(offset / jnp.float32(tap_reach))
    return jnp.where(inside, weights, jnp.zeros_like(weights))


def reference(traces, bin_steps):
    tap_reach = TAPS // 2
    bin_total = jnp.zeros((BI + 2, BX + 2, NT), jnp.float32)
    fold_count = jnp.zeros((BI + 2, BX + 2), jnp.float32)
    for row_phase in (0, 1):
        for col_phase in (0, 1):
            sub_traces = traces[row_phase::2, col_phase::2]
            step_il = bin_steps[0, row_phase::2, col_phase::2]
            step_xl = bin_steps[1, row_phase::2, col_phase::2]
            for shift_il in (-1, 0, 1):
                for shift_xl in (-1, 0, 1):
                    chosen = ((step_il == shift_il) & (step_xl == shift_xl)).astype(jnp.float32)
                    widths = ((1 + shift_il, 1 - shift_il), (1 + shift_xl, 1 - shift_xl))
                    bin_total = bin_total + jnp.pad(sub_traces * chosen[:, :, None], widths + ((0, 0),))
                    fold_count = fold_count + jnp.pad(chosen, widths)
    stacked = bin_total[1:-1, 1:-1] / jnp.maximum(fold_count[1:-1, 1:-1], 1.0)[:, :, None]
    padded = jnp.pad(stacked, ((0, 0), (0, 0), (tap_reach, tap_reach)))
    taps_table = lanczos_table(CT + 2 * tap_reach, CT * P_SIZE // Q, tap_reach, P_SIZE, Q)
    blocks = []
    for block_idx in range(N_TA):
        block_rows = padded[:, :, block_idx * CT: block_idx * CT + CT + 2 * tap_reach].reshape(BI * BX, CT + 2 * tap_reach)
        result = jnp.dot(block_rows, taps_table, precision=lax.Precision.HIGHEST, preferred_element_type=jnp.float32)
        blocks.append(result.reshape(BI, BX, CT * P_SIZE // Q))
    return jnp.concatenate(blocks, axis=2)
```

```python
import functools

import jax
import jax.numpy as jnp
import numpy as np
from jax import lax
from jax.experimental import pallas as pl
from jax.experimental.pallas import tpu as pltpu
from jax.sharding import PartitionSpec as P

TAPS = 16
P_SIZE = 3
Q = 2
REACH = TAPS // 2

LANES = 128
ROWS, COLS, SPAN = 16, 208, 256
BROWS, BCOLS, OUT = 8, 104, 384
HALF = 64
SPLIT = 56
LOW_RIM, HIGH_RIM = 56, 112
FIRST_BIN, LAST_BIN = 0, 111
WINDOWS = ((0, 120), (104, 208))
GROUPS = tuple(range(0, 56, 8)) + tuple(range(64, 112, 8))

OFFSETS = tuple(
    (di, dx, dt) for di in (0, 1) for dx in (-1, 0, 1) for dt in (-1, 0, 1) if (di, dx, dt) != (0, 0, 0)
)


def filter_table():
    lane = np.arange(LANES)
    sample = np.stack(
        [
            np.where(lane < 112, lane, lane - 128),
            np.where(lane < 64, lane + 128, lane),
            np.where(lane < 16, lane + 256, lane + 128),
        ]
    )
    output = np.arange(OUT).reshape(3, LANES)
    x = (Q * output[:, None, :] - P_SIZE * sample[:, :, None]) / P_SIZE
    weights = np.where(np.abs(x) < REACH, np.sinc(x) * np.sinc(x / REACH), 0.0).astype(np.float32)
    high = weights.astype(jnp.bfloat16)
    low = (weights - high.astype(np.float32)).astype(jnp.bfloat16)
    top = np.concatenate([high, low], axis=2)
    bottom = np.concatenate([high, np.zeros_like(low)], axis=2)
    return np.concatenate([top, bottom], axis=1)


def parts_of(values):
    high = values.astype(jnp.bfloat16)
    low = (values - high.astype(jnp.float32)).astype(jnp.bfloat16)
    return high, low


def both(*conditions):
    held = [c for c in conditions if c is not None]
    return functools.reduce(jnp.logical_and, held) if held else None


def guarded(condition, action):
    if condition is None:
        action()
    else:
        pl.when(condition)(action)


def kernel(
    n_xl, n_ta, traces, steps, table, out,
    x, sv, cbuf, tab, onehot, acc, rims, corner, packed, packed_rim,
    ra, rb, rc, rd, re, rf, rg, load_sem, send_sem, recv_sem,
):
    il, xl, ta = lax.axis_index("il"), lax.axis_index("xl"), lax.axis_index("ta")

    steps_copy = pltpu.make_async_copy(steps, sv, load_sem.at[0])
    steps_copy.start()
    loads = []
    for k in range(BROWS):
        rows = pl.ds(2 * k, 2)
        loads.append(pltpu.make_async_copy(traces.at[rows], x.at[rows], load_sem.at[k + 1]))
        loads[-1].start()
    table_copy = pltpu.make_async_copy(table, tab, load_sem.at[BROWS + 1])
    table_copy.start()

    def there(step, index, size):
        return None if step == 0 else (index > 0 if step < 0 else index < size - 1)

    def sends_to(offset):
        return both(there(offset[1], xl, n_xl), there(offset[2], ta, n_ta))

    def hears_from(offset):
        return both(there(-offset[1], xl, n_xl), there(-offset[2], ta, n_ta))

    def device(offset):
        return {"il": 1 - il if offset[0] else il, "xl": xl + offset[1], "ta": ta + offset[2]}

    barrier = pltpu.get_barrier_semaphore()
    for offset in OFFSETS:
        guarded(
            sends_to(offset),
            functools.partial(
                pl.semaphore_signal, barrier, 1, device_id=device(offset), device_id_type=pl.DeviceIdType.MESH
            ),
        )

    edge = (1 - il) * (BROWS + 1)
    target = BROWS - (BROWS - 1) * il

    copies, landing = {}, {}
    for number, offset in enumerate(OFFSETS):
        di, dx, dt = offset
        side, end = (dx + 1) // 2, (dt + 1) // 2
        lanes = pl.ds(LANES * end, LANES)
        if dt == 0 and dx == 0:
            source, place = acc.at[edge], ra
        elif dt == 0:
            source, place = (corner.at[side], rc.at[side]) if di else (rims.at[side], rb.at[side])
        elif dx == 0:
            source, place = (packed_rim.at[end], re.at[end]) if di else (packed.at[end], rd.at[end])
        elif di:
            source, place = corner.at[side, :, lanes], rg.at[end, side]
        else:
            source, place = rims.at[side, :, lanes], rf.at[end, side]
        landing[offset] = place
        copies[offset] = pltpu.make_async_remote_copy(
            src_ref=source,
            dst_ref=place,
            send_sem=send_sem.at[number],
            recv_sem=recv_sem.at[number],
            device_id=device(offset),
            device_id_type=pl.DeviceIdType.MESH,
        )

    for offset in OFFSETS:
        heard = hears_from(offset)
        if heard is not None:

            def clear(place=landing[offset]):
                place[...] = jnp.zeros(place.shape, jnp.float32)

            pl.when(jnp.logical_not(heard))(clear)

    steps_copy.wait()
    wide = lax.broadcasted_iota(jnp.int32, (ROWS, SPAN), 1)
    bin_col = lax.shift_right_logical(lax.broadcasted_iota(jnp.int32, (ROWS, COLS), 1), 1) + sv[1]
    base = (sv[0] + 1) * HALF
    cbuf[...] = jnp.full(cbuf.shape, -1, jnp.int32)
    cbuf[0, :, 0:COLS] = jnp.where(
        bin_col < 0, base + LOW_RIM, jnp.where(bin_col < SPLIT, base + bin_col, -1)
    )
    cbuf[1, :, 0:COLS] = jnp.where(bin_col >= SPLIT, base + bin_col - SPLIT, -1)
    first, second = cbuf[0], cbuf[1]
    codes = (
        (
            jnp.where(wide < 120, first, -1),
            jnp.where((wide >= 120) & (wide < 240), pltpu.roll(first, 120, 1), -1),
        ),
        (
            jnp.where(wide < 104, pltpu.roll(second, SPAN - 104, 1), -1),
            jnp.where((wide >= 104) & (wide < 208), second, -1),
        ),
    )
    places = lax.broadcasted_iota(jnp.int32, (3 * HALF, SPAN), 0)
    for k in range(BROWS):
        for h in range(2):
            even, odd = codes[h]
            code = jnp.maximum(even[2 * k : 2 * k + 1], odd[2 * k + 1 : 2 * k + 2])
            chosen = jnp.where(places == code, 1.0, 0.0)
            onehot[k, h] = chosen.astype(jnp.bfloat16)
            counts = jnp.broadcast_to(jnp.sum(chosen, axis=1, keepdims=True), (3 * HALF, LANES))
            for q in range(3):
                b = k + q
                where = (b, pl.ds(HALF * h, HALF), pl.ds(SPAN, LANES))
                part = counts[HALF * q : HALF * (q + 1)]
                acc[where] = part if k == max(b - 2, 0) else acc[where] + part

    lane = lax.broadcasted_iota(jnp.int32, (8, LANES), 1)

    def in_group(r, end):
        start = (8 * r + (120 if end else 0)) % LANES
        return (lane >= start) & (lane < start + 8)

    def pack(b, end):
        tile = pl.ds(LANES * end, LANES)
        total = acc[b, 0:8, tile]
        for r in range(1, len(GROUPS)):
            turned = pltpu.roll(acc[b, GROUPS[r] : GROUPS[r] + 8, tile], 8 * r, 1)
            total = jnp.where(in_group(r, end), turned, total)
        return total

    def finish(b):
        for end in (0, 1):
            packed[end, b - 1] = pack(b, end)
        for side, row in ((0, LOW_RIM), (1, HIGH_RIM)):
            rims[side, b - 1 : b, :] = acc[b, row : row + 1, :]

    for k in range(BROWS):
        loads[k].wait()
        for h in range(2):
            start, stop = WINDOWS[h]
            pieces = [x[2 * k, start:stop, :], x[2 * k + 1, start:stop, :]]
            pieces.append(jnp.zeros((SPAN - 2 * (stop - start), SPAN), jnp.float32))
            high, low = parts_of(jnp.concatenate(pieces, axis=0))
            chosen = onehot[k, h]
            result = jnp.dot(chosen, high, preferred_element_type=jnp.float32)
            result = result + jnp.dot(chosen, low, preferred_element_type=jnp.float32)
            for q in range(3):
                b = k + q
                where = (b, pl.ds(HALF * h, HALF), pl.ds(0, SPAN))
                part = result[HALF * q : HALF * (q + 1)]
                acc[where] = part if k == max(b - 2, 0) else acc[where] + part
        if k > 0:
            finish(k)
    finish(BROWS)
    for end in (0, 1):
        packed_rim[end] = pack(edge, end)
    for side, row in ((0, LOW_RIM), (1, HIGH_RIM)):
        corner[side] = jnp.broadcast_to(acc[edge, row : row + 1, :], (8, OUT))

    beside_xl = 1 + (xl > 0).astype(jnp.int32) + (xl < n_xl - 1).astype(jnp.int32)
    beside_ta = 1 + (ta > 0).astype(jnp.int32) + (ta < n_ta - 1).astype(jnp.int32)
    pl.semaphore_wait(barrier, 2 * beside_xl * beside_ta - 1)
    for offset in sorted(OFFSETS, key=lambda o: -abs(o[2])):
        guarded(sends_to(offset), copies[offset].start)

    def heard(*offsets):
        for offset in offsets:
            guarded(hears_from(offset), copies[offset].wait_recv)

    heard((1, 0, 0), (0, -1, 0), (0, 1, 0), (1, -1, 0), (1, 1, 0))
    acc[target] = acc[target] + ra[...]
    for row, side in ((FIRST_BIN, 1), (LAST_BIN, 0)):
        acc[target, row : row + 1, :] = acc[target, row : row + 1, :] + rc[side, 0:1, :]
        for b in range(BROWS):
            acc[b + 1, row : row + 1, :] = acc[b + 1, row : row + 1, :] + rb[side, b : b + 1, :]

    table_copy.wait()

    def bins(b, tile):
        lanes = pl.ds(LANES * tile, LANES)
        return [acc[b, 0:SPLIT, lanes], acc[b, HALF : HALF + BCOLS - SPLIT, lanes]]

    def pair(p, tile):
        return jnp.concatenate(bins(2 * p + 1, tile) + bins(2 * p + 2, tile), axis=0)

    across = lax.broadcasted_iota(jnp.int32, (2 * BCOLS, LANES), 1)

    def resample(p, third, window):
        high, low = parts_of(window)
        result = jnp.dot(
            jnp.concatenate([high, low], axis=1), tab[third], preferred_element_type=jnp.float32
        )
        result = result[:, :LANES] + result[:, LANES:]
        lanes = pl.ds(LANES * third, LANES)
        out[2 * p, :, lanes] = result[:BCOLS]
        out[2 * p + 1, :, lanes] = result[BCOLS:]

    scales = []
    for p in range(BROWS // 2):
        scales.append(1.0 / jnp.maximum(pair(p, 2), 1.0))
        resample(p, 1, jnp.where(across < 64, pair(p, 1), pair(p, 0)) * scales[p])

    for end in (1, 0):
        dt = 2 * end - 1
        heard((0, 0, dt), (1, 0, dt), (0, -1, dt), (0, 1, dt), (1, -1, dt), (1, 1, dt))
        rd[end, target - 1] = rd[end, target - 1] + re[end]
        for sublane, r, side in ((0, 0, 1), (7, len(GROUPS) - 1, 0)):
            mask = in_group(r, end)
            near = jnp.where(mask, pltpu.roll(rf[end, side], 8 * r, 1) if r else rf[end, side], 0.0)
            far = jnp.where(mask, pltpu.roll(rg[end, side], 8 * r, 1) if r else rg[end, side], 0.0)
            row = slice(sublane, sublane + 1)
            rd[end, target - 1, row, :] = rd[end, target - 1, row, :] + far[0:1]
            for b in range(BROWS):
                rd[end, b, row, :] = rd[end, b, row, :] + near[b : b + 1]
        for p in range(BROWS // 2):
            halo = []
            for b in (2 * p, 2 * p + 1):
                tile = rd[end, b]
                halo += [pltpu.roll(tile, LANES - 8 * r, 1) if r else tile for r in range(len(GROUPS))]
            halo = jnp.concatenate(halo, axis=0)
            if end:
                window = jnp.where(across < 112, pair(p, 0), halo)
                resample(p, 0, window * scales[p])
            else:
                window = jnp.where(across < 16, halo, pair(p, 1))
                resample(p, 2, window * scales[p])

    for offset in OFFSETS:
        guarded(sends_to(offset), copies[offset].wait_send)


def solution(mesh):
    n_xl, n_ta = mesh.shape["xl"], mesh.shape["ta"]
    table = filter_table()
    f32 = jnp.float32

    def shards(traces, steps):
        return pl.pallas_call(
            functools.partial(kernel, n_xl, n_ta),
            name="stack_resample",
            out_shape=jax.ShapeDtypeStruct((BROWS, BCOLS, OUT), f32),
            in_specs=[pl.BlockSpec(memory_space=pltpu.HBM)] * 3,
            out_specs=pl.BlockSpec(memory_space=pltpu.VMEM),
            scratch_shapes=[
                pltpu.VMEM((ROWS, COLS, SPAN), f32),
                pltpu.VMEM((2, ROWS, COLS), jnp.int32),
                pltpu.VMEM((2, ROWS, SPAN), jnp.int32),
                pltpu.VMEM((3, SPAN, SPAN), jnp.bfloat16),
                pltpu.VMEM((BROWS, 2, 3 * HALF, SPAN), jnp.bfloat16),
                pltpu.VMEM((BROWS + 2, 2 * HALF, OUT), f32),
                pltpu.VMEM((2, BROWS, OUT), f32),
                pltpu.VMEM((2, 8, OUT), f32),
                pltpu.VMEM((2, BROWS, 8, LANES), f32),
                pltpu.VMEM((2, 8, LANES), f32),
                pltpu.VMEM((2 * HALF, OUT), f32),
                pltpu.VMEM((2, BROWS, OUT), f32),
                pltpu.VMEM((2, 8, OUT), f32),
                pltpu.VMEM((2, BROWS, 8, LANES), f32),
                pltpu.VMEM((2, 8, LANES), f32),
                pltpu.VMEM((2, 2, BROWS, LANES), f32),
                pltpu.VMEM((2, 2, 8, LANES), f32),
                pltpu.SemaphoreType.DMA((BROWS + 2,)),
                pltpu.SemaphoreType.DMA((len(OFFSETS),)),
                pltpu.SemaphoreType.DMA((len(OFFSETS),)),
            ],
            compiler_params=pltpu.CompilerParams(
                collective_id=0, has_side_effects=True, vmem_limit_bytes=32 * 1024 * 1024
            ),
        )(traces, steps, table)

    return jax.shard_map(
        shards,
        mesh=mesh,
        in_specs=(P("il", "xl", "ta"), P(None, "il", "xl")),
        out_specs=P("il", "xl", "ta"),
        check_vma=False,
    )
```

```python
import functools

import jax
import jax.numpy as jnp
import numpy as np
from jax import lax
from jax.experimental import pallas as pl
from jax.experimental.pallas import tpu as pltpu
from jax.sharding import PartitionSpec as P

TAPS = 16
P_SIZE = 3
Q = 2
REACH = TAPS // 2

LANES = 128
ROWS, COLS, SPAN = 16, 208, 256
BROWS, BCOLS, OUT = 8, 104, 384
HALF = 64
SPLIT = 56
LOW_RIM, HIGH_RIM = 56, 112
FIRST_BIN, LAST_BIN = 0, 111
WINDOWS = ((0, 120), (104, 208))
GROUPS = tuple(range(0, 56, 8)) + tuple(range(64, 112, 8))

OFFSETS = tuple(
    (di, dx, dt) for di in (0, 1) for dx in (-1, 0, 1) for dt in (-1, 0, 1) if (di, dx, dt) != (0, 0, 0)
)


def filter_table():
    lane = np.arange(LANES)
    sample = np.stack(
        [
            np.where(lane < 112, lane, lane - 128),
            np.where(lane < 64, lane + 128, lane),
            np.where(lane < 16, lane + 256, lane + 128),
        ]
    )
    output = np.arange(OUT).reshape(3, LANES)
    x = (Q * output[:, None, :] - P_SIZE * sample[:, :, None]) / P_SIZE
    weights = np.where(np.abs(x) < REACH, np.sinc(x) * np.sinc(x / REACH), 0.0).astype(np.float32)
    high = weights.astype(jnp.bfloat16)
    low = (weights - high.astype(np.float32)).astype(jnp.bfloat16)
    top = np.concatenate([high, low], axis=2)
    bottom = np.concatenate([high, np.zeros_like(low)], axis=2)
    return np.concatenate([top, bottom], axis=1)


def parts_of(values):
    high = values.astype(jnp.bfloat16)
    low = (values - high.astype(jnp.float32)).astype(jnp.bfloat16)
    return high, low


def both(*conditions):
    held = [c for c in conditions if c is not None]
    return functools.reduce(jnp.logical_and, held) if held else None


def guarded(condition, action):
    if condition is None:
        action()
    else:
        pl.when(condition)(action)


def kernel(
    n_xl, n_ta, traces, steps, table, out,
    x, sv, cbuf, tab, onehot, acc, rims, corner, packed, packed_rim,
    ra, rb, rc, rd, re, rf, rg, load_sem, send_sem, recv_sem,
):
    il, xl, ta = lax.axis_index("il"), lax.axis_index("xl"), lax.axis_index("ta")

    steps_copy = pltpu.make_async_copy(steps, sv, load_sem.at[0])
    steps_copy.start()
    loads = []
    for k in range(BROWS):
        rows = pl.ds(2 * k, 2)
        loads.append(pltpu.make_async_copy(traces.at[rows], x.at[rows], load_sem.at[k + 1]))
        loads[-1].start()
    table_copy = pltpu.make_async_copy(table, tab, load_sem.at[BROWS + 1])
    table_copy.start()

    def there(step, index, size):
        return None if step == 0 else (index > 0 if step < 0 else index < size - 1)

    def sends_to(offset):
        return both(there(offset[1], xl, n_xl), there(offset[2], ta, n_ta))

    def hears_from(offset):
        return both(there(-offset[1], xl, n_xl), there(-offset[2], ta, n_ta))

    def device(offset):
        return {"il": 1 - il if offset[0] else il, "xl": xl + offset[1], "ta": ta + offset[2]}

    barrier = pltpu.get_barrier_semaphore()
    for offset in OFFSETS:
        guarded(
            sends_to(offset),
            functools.partial(
                pl.semaphore_signal, barrier, 1, device_id=device(offset), device_id_type=pl.DeviceIdType.MESH
            ),
        )

    edge = (1 - il) * (BROWS + 1)
    target = BROWS - (BROWS - 1) * il

    copies, landing = {}, {}
    for number, offset in enumerate(OFFSETS):
        di, dx, dt = offset
        side, end = (dx + 1) // 2, (dt + 1) // 2
        lanes = pl.ds(LANES * end, LANES)
        if dt == 0 and dx == 0:
            source, place = acc.at[edge], ra
        elif dt == 0:
            source, place = (corner.at[side], rc.at[side]) if di else (rims.at[side], rb.at[side])
        elif dx == 0:
            source, place = (packed_rim.at[end], re.at[end]) if di else (packed.at[end], rd.at[end])
        elif di:
            source, place = corner.at[side, :, lanes], rg.at[end, side]
        else:
            source, place = rims.at[side, :, lanes], rf.at[end, side]
        landing[offset] = place
        copies[offset] = pltpu.make_async_remote_copy(
            src_ref=source,
            dst_ref=place,
            send_sem=send_sem.at[number],
            recv_sem=recv_sem.at[number],
            device_id=device(offset),
            device_id_type=pl.DeviceIdType.MESH,
        )

    for offset in OFFSETS:
        heard = hears_from(offset)
        if heard is not None:

            def clear(place=landing[offset]):
                place[...] = jnp.zeros(place.shape, jnp.float32)

            pl.when(jnp.logical_not(heard))(clear)

    steps_copy.wait()
    wide = lax.broadcasted_iota(jnp.int32, (ROWS, SPAN), 1)
    bin_col = lax.shift_right_logical(lax.broadcasted_iota(jnp.int32, (ROWS, COLS), 1), 1) + sv[1]
    base = (sv[0] + 1) * HALF
    cbuf[...] = jnp.full(cbuf.shape, -1, jnp.int32)
    cbuf[0, :, 0:COLS] = jnp.where(
        bin_col < 0, base + LOW_RIM, jnp.where(bin_col < SPLIT, base + bin_col, -1)
    )
    cbuf[1, :, 0:COLS] = jnp.where(bin_col >= SPLIT, base + bin_col - SPLIT, -1)
    first, second = cbuf[0], cbuf[1]
    codes = (
        (
            jnp.where(wide < 120, first, -1),
            jnp.where((wide >= 120) & (wide < 240), pltpu.roll(first, 120, 1), -1),
        ),
        (
            jnp.where(wide < 104, pltpu.roll(second, SPAN - 104, 1), -1),
            jnp.where((wide >= 104) & (wide < 208), second, -1),
        ),
    )
    places = lax.broadcasted_iota(jnp.int32, (3 * HALF, SPAN), 0)
    for k in range(BROWS):
        for h in range(2):
            even, odd = codes[h]
            code = jnp.maximum(even[2 * k : 2 * k + 1], odd[2 * k + 1 : 2 * k + 2])
            chosen = jnp.where(places == code, 1.0, 0.0)
            onehot[k, h] = chosen.astype(jnp.bfloat16)
            counts = jnp.broadcast_to(jnp.sum(chosen, axis=1, keepdims=True), (3 * HALF, LANES))
            for q in range(3):
                b = k + q
                where = (b, pl.ds(HALF * h, HALF), pl.ds(SPAN, LANES))
                part = counts[HALF * q : HALF * (q + 1)]
                acc[where] = part if k == max(b - 2, 0) else acc[where] + part

    lane = lax.broadcasted_iota(jnp.int32, (8, LANES), 1)

    def in_group(r, end):
        start = (8 * r + (120 if end else 0)) % LANES
        return (lane >= start) & (lane < start + 8)

    def pack(b, end):
        tile = pl.ds(LANES * end, LANES)
        total = acc[b, 0:8, tile]
        for r in range(1, len(GROUPS)):
            turned = pltpu.roll(acc[b, GROUPS[r] : GROUPS[r] + 8, tile], 8 * r, 1)
            total = jnp.where(in_group(r, end), turned, total)
        return total

    def finish(b):
        for end in (0, 1):
            packed[end, b - 1] = pack(b, end)
        for side, row in ((0, LOW_RIM), (1, HIGH_RIM)):
            rims[side, b - 1 : b, :] = acc[b, row : row + 1, :]

    for k in range(BROWS):
        loads[k].wait()
        for h in range(2):
            start, stop = WINDOWS[h]
            pieces = [x[2 * k, start:stop, :], x[2 * k + 1, start:stop, :]]
            pieces.append(jnp.zeros((SPAN - 2 * (stop - start), SPAN), jnp.float32))
            high, low = parts_of(jnp.concatenate(pieces, axis=0))
            chosen = onehot[k, h]
            result = jnp.dot(chosen, high, preferred_element_type=jnp.float32)
            result = result + jnp.dot(chosen, low, preferred_element_type=jnp.float32)
            for q in range(3):
                b = k + q
                where = (b, pl.ds(HALF * h, HALF), pl.ds(0, SPAN))
                part = result[HALF * q : HALF * (q + 1)]
                acc[where] = part if k == max(b - 2, 0) else acc[where] + part
        if k > 0:
            finish(k)
    finish(BROWS)
    for end in (0, 1):
        packed_rim[end] = pack(edge, end)
    for side, row in ((0, LOW_RIM), (1, HIGH_RIM)):
        corner[side] = jnp.broadcast_to(acc[edge, row : row + 1, :], (8, OUT))

    beside_xl = 1 + (xl > 0).astype(jnp.int32) + (xl < n_xl - 1).astype(jnp.int32)
    beside_ta = 1 + (ta > 0).astype(jnp.int32) + (ta < n_ta - 1).astype(jnp.int32)
    pl.semaphore_wait(barrier, 2 * beside_xl * beside_ta - 1)
    for offset in sorted(OFFSETS, key=lambda o: -abs(o[2])):
        guarded(sends_to(offset), copies[offset].start)

    def heard(*offsets):
        for offset in offsets:
            guarded(hears_from(offset), copies[offset].wait_recv)

    heard((1, 0, 0), (0, -1, 0), (0, 1, 0), (1, -1, 0), (1, 1, 0))
    acc[target] = acc[target] + ra[...]
    for row, side in ((FIRST_BIN, 1), (LAST_BIN, 0)):
        acc[target, row : row + 1, :] = acc[target, row : row + 1, :] + rc[side, 0:1, :]
        for b in range(BROWS):
            acc[b + 1, row : row + 1, :] = acc[b + 1, row : row + 1, :] + rb[side, b : b + 1, :]

    table_copy.wait()

    def bins(b, tile):
        lanes = pl.ds(LANES * tile, LANES)
        return [acc[b, 0:SPLIT, lanes], acc[b, HALF : HALF + BCOLS - SPLIT, lanes]]

    def pair(p, tile):
        return jnp.concatenate(bins(2 * p + 1, tile) + bins(2 * p + 2, tile), axis=0)

    across = lax.broadcasted_iota(jnp.int32, (2 * BCOLS, LANES), 1)

    def resample(p, third, window):
        high, low = parts_of(window)
        result = jnp.dot(
            jnp.concatenate([high, low], axis=1), tab[third], preferred_element_type=jnp.float32
        )
        result = result[:, :LANES] + result[:, LANES:]
        lanes = pl.ds(LANES * third, LANES)
        out[2 * p, :, lanes] = result[:BCOLS]
        out[2 * p + 1, :, lanes] = result[BCOLS:]

    scales = []
    for p in range(BROWS // 2):
        scales.append(1.0 / jnp.maximum(pair(p, 2), 1.0))
        resample(p, 1, jnp.where(across < 64, pair(p, 1), pair(p, 0)) * scales[p])

    for end in (1, 0):
        dt = 2 * end - 1
        heard((0, 0, dt), (1, 0, dt), (0, -1, dt), (0, 1, dt), (1, -1, dt), (1, 1, dt))
        rd[end, target - 1] = rd[end, target - 1] + re[end]
        for sublane, r, side in ((0, 0, 1), (7, len(GROUPS) - 1, 0)):
            mask = in_group(r, end)
            near = jnp.where(mask, pltpu.roll(rf[end, side], 8 * r, 1) if r else rf[end, side], 0.0)
            far = jnp.where(mask, pltpu.roll(rg[end, side], 8 * r, 1) if r else rg[end, side], 0.0)
            row = slice(sublane, sublane + 1)
            rd[end, target - 1, row, :] = rd[end, target - 1, row, :] + far[0:1]
            for b in range(BROWS):
                rd[end, b, row, :] = rd[end, b, row, :] + near[b : b + 1]
        for p in range(BROWS // 2):
            halo = []
            for b in (2 * p, 2 * p + 1):
                tile = rd[end, b]
                halo += [pltpu.roll(tile, LANES - 8 * r, 1) if r else tile for r in range(len(GROUPS))]
            halo = jnp.concatenate(halo, axis=0)
            if end:
                window = jnp.where(across < 112, pair(p, 0), halo)
                resample(p, 0, window * scales[p])
            else:
                window = jnp.where(across < 16, halo, pair(p, 1))
                resample(p, 2, window * scales[p])

    for offset in OFFSETS:
        guarded(sends_to(offset), copies[offset].wait_send)


def solution(mesh):
    n_xl, n_ta = mesh.shape["xl"], mesh.shape["ta"]
    table = filter_table()
    f32 = jnp.float32

    def shards(traces, steps):
        return pl.pallas_call(
            functools.partial(kernel, n_xl, n_ta),
            name="stack_resample",
            out_shape=jax.ShapeDtypeStruct((BROWS, BCOLS, OUT), f32),
            in_specs=[pl.BlockSpec(memory_space=pltpu.HBM)] * 3,
            out_specs=pl.BlockSpec(memory_space=pltpu.VMEM),
            scratch_shapes=[
                pltpu.VMEM((ROWS, COLS, SPAN), f32),
                pltpu.VMEM((2, ROWS, COLS), jnp.int32),
                pltpu.VMEM((2, ROWS, SPAN), jnp.int32),
                pltpu.VMEM((3, SPAN, SPAN), jnp.bfloat16),
                pltpu.VMEM((BROWS, 2, 3 * HALF, SPAN), jnp.bfloat16),
                pltpu.VMEM((BROWS + 2, 2 * HALF, OUT), f32),
                pltpu.VMEM((2, BROWS, OUT), f32),
                pltpu.VMEM((2, 8, OUT), f32),
                pltpu.VMEM((2, BROWS, 8, LANES), f32),
                pltpu.VMEM((2, 8, LANES), f32),
                pltpu.VMEM((2 * HALF, OUT), f32),
                pltpu.VMEM((2, BROWS, OUT), f32),
                pltpu.VMEM((2, 8, OUT), f32),
                pltpu.VMEM((2, BROWS, 8, LANES), f32),
                pltpu.VMEM((2, 8, LANES), f32),
                pltpu.VMEM((2, 2, BROWS, LANES), f32),
                pltpu.VMEM((2, 2, 8, LANES), f32),
                pltpu.SemaphoreType.DMA((BROWS + 2,)),
                pltpu.SemaphoreType.DMA((len(OFFSETS),)),
                pltpu.SemaphoreType.DMA((len(OFFSETS),)),
            ],
            compiler_params=pltpu.CompilerParams(
                collective_id=0, has_side_effects=True, vmem_limit_bytes=32 * 1024 * 1024
            ),
        )(*(pltpu.with_memory_space_constraint(a, pltpu.HBM) for a in (traces, steps, jnp.asarray(table))))

    return jax.shard_map(
        shards,
        mesh=mesh,
        in_specs=(P("il", "xl", "ta"), P(None, "il", "xl")),
        out_specs=P("il", "xl", "ta"),
        check_vma=False,
    )
```

```python
import functools

import jax
import jax.numpy as jnp
import numpy as np
from jax import lax
from jax.experimental import pallas as pl
from jax.experimental.pallas import tpu as pltpu
from jax.sharding import PartitionSpec as P

TAPS = 16
P_SIZE = 3
Q = 2
REACH = TAPS // 2

LANES = 128
ROWS, COLS, SPAN = 16, 208, 256
BROWS, BCOLS, OUT = 8, 104, 384
HALF = 64
SPLIT = 56
LOW_RIM, HIGH_RIM = 56, 112
FIRST_BIN, LAST_BIN = 0, 111
WINDOWS = ((0, 120), (104, 208))
GROUPS = tuple(range(0, 56, 8)) + tuple(range(64, 112, 8))

OFFSETS = tuple(
    (di, dx, dt) for di in (0, 1) for dx in (-1, 0, 1) for dt in (-1, 0, 1) if (di, dx, dt) != (0, 0, 0)
)


SIDES = ((-1, -1), (-1, 1), (1, -1), (1, 1), (0, -1), (0, 1), (-1, 0), (1, 0), (0, 0))


def filter_table():
    lane = np.arange(LANES)
    sample = np.stack(
        [
            np.where(lane < 112, lane, lane - 128),
            np.where(lane < 64, lane + 128, lane),
            np.where(lane < 16, lane + 256, lane + 128),
        ]
    )
    output = np.arange(OUT).reshape(3, LANES)
    x = (Q * output[:, None, :] - P_SIZE * sample[:, :, None]) / P_SIZE
    weights = np.where(np.abs(x) < REACH, np.sinc(x) * np.sinc(x / REACH), 0.0).astype(np.float32)
    high = weights.astype(jnp.bfloat16)
    low = (weights - high.astype(np.float32)).astype(jnp.bfloat16)
    top = np.concatenate([high, low], axis=2)
    bottom = np.concatenate([high, np.zeros_like(low)], axis=2)
    return np.concatenate([top, bottom], axis=1)


def parts_of(values):
    high = values.astype(jnp.bfloat16)
    low = (values - high.astype(jnp.float32)).astype(jnp.bfloat16)
    return high, low


def both(*conditions):
    held = [c for c in conditions if c is not None]
    return functools.reduce(jnp.logical_and, held) if held else None


def kernel(
    n_xl, n_ta, traces, steps, table, out,
    x, sv, cbuf, tab, onehot, acc, scale, rims, corner, packed, packed_rim,
    ra, rb, rc, rd, re, rf, rg, load_sem, send_sem, recv_sem,
):
    il, xl, ta = lax.axis_index("il"), lax.axis_index("xl"), lax.axis_index("ta")

    def there(step, index, size):
        return None if step == 0 else (index > 0 if step < 0 else index < size - 1)

    def device(offset):
        return {"il": 1 - il if offset[0] else il, "xl": xl + offset[1], "ta": ta + offset[2]}

    def for_neighbours(sides, action, sign=1):
        for dx, dt in sides:
            condition = both(there(sign * dx, xl, n_xl), there(sign * dt, ta, n_ta))

            def run(dx=dx, dt=dt):
                for di in (0, 1):
                    if (di, dx, dt) != (0, 0, 0):
                        action((di, dx, dt))

            if condition is None:
                run()
            else:
                pl.when(condition)(run)

    barrier = pltpu.get_barrier_semaphore()

    def greet(offset):
        pl.semaphore_signal(
            barrier, 1, device_id=device(offset), device_id_type=pl.DeviceIdType.MESH
        )

    for_neighbours(SIDES, greet)

    steps_copy = pltpu.make_async_copy(steps, sv, load_sem.at[0])
    steps_copy.start()
    loads = []
    for k in range(BROWS):
        rows = pl.ds(2 * k, 2)
        loads.append(pltpu.make_async_copy(traces.at[rows], x.at[rows], load_sem.at[k + 1]))
        loads[-1].start()
    table_copy = pltpu.make_async_copy(table, tab, load_sem.at[BROWS + 1])
    table_copy.start()

    edge = (1 - il) * (BROWS + 1)
    target = BROWS - (BROWS - 1) * il

    copies = {}
    for number, offset in enumerate(OFFSETS):
        di, dx, dt = offset
        side, end = (dx + 1) // 2, (dt + 1) // 2
        lanes = pl.ds(LANES * end, LANES)
        if dt == 0 and dx == 0:
            rows = pl.ds(0, LAST_BIN + 1)
            source, place = acc.at[edge, rows], ra
        elif dt == 0:
            source, place = (corner.at[side], rc.at[side]) if di else (rims.at[side], rb.at[side])
        elif dx == 0:
            source, place = (packed_rim.at[end], re.at[end]) if di else (packed.at[end], rd.at[end])
        elif di:
            source, place = corner.at[side, :, lanes], rg.at[end, side]
        else:
            source, place = rims.at[side, :, lanes], rf.at[end, side]
        copies[offset] = pltpu.make_async_remote_copy(
            src_ref=source,
            dst_ref=place,
            send_sem=send_sem.at[number],
            recv_sem=recv_sem.at[number],
            device_id=device(offset),
            device_id_type=pl.DeviceIdType.MESH,
        )

    for dx in (-1, 1):
        side = (dx + 1) // 2

        @pl.when(jnp.logical_not(there(-dx, xl, n_xl)))
        def _(side=side):
            for place in (rb.at[side], rc.at[side], *(r.at[e, side] for r in (rf, rg) for e in (0, 1))):
                place[...] = jnp.zeros(place.shape, jnp.float32)

    for dt in (-1, 1):
        end = (dt + 1) // 2

        @pl.when(jnp.logical_not(there(-dt, ta, n_ta)))
        def _(end=end):
            for place in (rd.at[end], re.at[end], rf.at[end], rg.at[end]):
                place[...] = jnp.zeros(place.shape, jnp.float32)

    steps_copy.wait()
    wide = lax.broadcasted_iota(jnp.int32, (ROWS, SPAN), 1)
    bin_col = lax.shift_right_logical(lax.broadcasted_iota(jnp.int32, (ROWS, COLS), 1), 1) + sv[1]
    base = (sv[0] + 1) * HALF
    cbuf[...] = jnp.full(cbuf.shape, -1, jnp.int32)
    cbuf[0, :, 0:COLS] = jnp.where(
        bin_col < 0, base + LOW_RIM, jnp.where(bin_col < SPLIT, base + bin_col, -1)
    )
    cbuf[1, :, 0:COLS] = jnp.where(bin_col >= SPLIT, base + bin_col - SPLIT, -1)
    first, second = cbuf[0], cbuf[1]
    codes = (
        (
            jnp.where(wide < 120, first, -1),
            jnp.where((wide >= 120) & (wide < 240), pltpu.roll(first, 120, 1), -1),
        ),
        (
            jnp.where(wide < 104, pltpu.roll(second, SPAN - 104, 1), -1),
            jnp.where((wide >= 104) & (wide < 208), second, -1),
        ),
    )
    places = lax.broadcasted_iota(jnp.int32, (3 * HALF, SPAN), 0)
    for k in range(BROWS):
        for h in range(2):
            even, odd = codes[h]
            code = jnp.maximum(even[2 * k : 2 * k + 1], odd[2 * k + 1 : 2 * k + 2])
            onehot[k, h] = jnp.where(places == code, 1.0, 0.0).astype(jnp.bfloat16)

    for b in range(BROWS + 2):
        for h in range(2):
            rows = [onehot[k, h, HALF * (b - k) : HALF * (b - k + 1), :] for k in range(BROWS) if 0 <= b - k < 3]
            total = functools.reduce(jnp.add, rows)
            total = (total[:, :LANES] + total[:, LANES:]).astype(jnp.float32)
            acc[b, HALF * h : HALF * (h + 1), SPAN:OUT] = jnp.broadcast_to(
                jnp.sum(total, axis=1, keepdims=True), (HALF, LANES)
            )

    lane = lax.broadcasted_iota(jnp.int32, (8, LANES), 1)
    sublane = lax.broadcasted_iota(jnp.int32, (8, LANES), 0)

    def in_group(r, end):
        start = (8 * r + (120 if end else 0)) % LANES
        return (lane >= start) & (lane < start + 8)

    def pack(b, end):
        tile = pl.ds(LANES * end, LANES)
        total = acc[b, 0:8, tile]
        for r in range(1, len(GROUPS)):
            turned = pltpu.roll(acc[b, GROUPS[r] : GROUPS[r] + 8, tile], 8 * r, 1)
            total = jnp.where(in_group(r, end), turned, total)
        return total

    def finish(b):
        for side, row in ((0, LOW_RIM), (1, HIGH_RIM)):
            rims[side, b - 1 : b, :] = acc[b, row : row + 1, :]
        for end in (0, 1):
            packed[end, b - 1] = pack(b, end)

    for block in (range(0, 4), range(4, 8)):
        for k in block:
            loads[k].wait()
        for k in block:
            for h in range(2):
                start, stop = WINDOWS[h]
                pieces = [x[2 * k, start:stop, :], x[2 * k + 1, start:stop, :]]
                pieces.append(jnp.zeros((SPAN - 2 * (stop - start), SPAN), jnp.float32))
                high, low = parts_of(jnp.concatenate(pieces, axis=0))
                chosen = onehot[k, h]
                result = jnp.dot(chosen, high, preferred_element_type=jnp.float32)
                result = result + jnp.dot(chosen, low, preferred_element_type=jnp.float32)
                for q in range(3):
                    b = k + q
                    where = (b, pl.ds(HALF * h, HALF), pl.ds(0, SPAN))
                    part = result[HALF * q : HALF * (q + 1)]
                    acc[where] = part if k == max(b - 2, 0) else acc[where] + part
            if k > 0:
                finish(k)
    finish(BROWS)
    for side, row in ((0, LOW_RIM), (1, HIGH_RIM)):
        corner[side] = acc[edge, row : row + 1, :]
    for end in (0, 1):
        packed_rim[end] = pack(edge, end)

    beside_xl = 1 + (xl > 0).astype(jnp.int32) + (xl < n_xl - 1).astype(jnp.int32)
    beside_ta = 1 + (ta > 0).astype(jnp.int32) + (ta < n_ta - 1).astype(jnp.int32)
    pl.semaphore_wait(barrier, 2 * beside_xl * beside_ta - 1)
    for_neighbours(SIDES, lambda offset: copies[offset].start())

    for_neighbours(SIDES[6:], lambda offset: copies[offset].wait_recv(), -1)
    acc[target, 0 : LAST_BIN + 1, :] = acc[target, 0 : LAST_BIN + 1, :] + ra[...]
    for row, side in ((FIRST_BIN, 1), (LAST_BIN, 0)):
        acc[target, row : row + 1, :] = acc[target, row : row + 1, :] + rc[side]
        for b in range(BROWS):
            acc[b + 1, row : row + 1, :] = acc[b + 1, row : row + 1, :] + rb[side, b : b + 1, :]

    table_copy.wait()

    def bins(b, tile):
        lanes = pl.ds(LANES * tile, LANES)
        return [acc[b, 0:SPLIT, lanes], acc[b, HALF : HALF + BCOLS - SPLIT, lanes]]

    def pair(p, tile):
        return jnp.concatenate(bins(2 * p + 1, tile) + bins(2 * p + 2, tile), axis=0)

    across = lax.broadcasted_iota(jnp.int32, (2 * BCOLS, LANES), 1)

    def resample(p, third, window):
        high, low = parts_of(window)
        result = jnp.dot(
            jnp.concatenate([high, low], axis=1), tab[third], preferred_element_type=jnp.float32
        )
        result = result[:, :LANES] + result[:, LANES:]
        lanes = pl.ds(LANES * third, LANES)
        out[2 * p, :, lanes] = result[:BCOLS]
        out[2 * p + 1, :, lanes] = result[BCOLS:]

    for p in range(BROWS // 2):
        scale[p] = 1.0 / jnp.maximum(pair(p, 2), 1.0)
        resample(p, 1, jnp.where(across < 64, pair(p, 1), pair(p, 0)) * scale[p])

    for_neighbours(SIDES[:6], lambda offset: copies[offset].wait_recv(), -1)

    def halo(end):
        last = len(GROUPS) - 1
        here = in_group(0, end), in_group(last, end)
        near = [jnp.where(here[0], rf[end, 1], 0.0), jnp.where(here[1], pltpu.roll(rf[end, 0], 8 * last, 1), 0.0)]
        far = jnp.where(here[0] & (sublane == 0), rg[end, 1], 0.0)
        turned = pltpu.roll(jnp.broadcast_to(rg[end, 0], (8, LANES)), 8 * last, 1)
        far = far + jnp.where(here[1] & (sublane == 7), turned, 0.0) + re[end]
        rows = []
        for b in range(BROWS):
            tile = rd[end, b]
            tile = tile + jnp.where(sublane == 0, near[0][b : b + 1], 0.0)
            tile = tile + jnp.where(sublane == 7, near[1][b : b + 1], 0.0)
            if b in (0, BROWS - 1):
                tile = tile + jnp.where(target == b + 1, far, 0.0)
            rows += [pltpu.roll(tile, LANES - 8 * r, 1) if r else tile for r in range(len(GROUPS))]
        return rows

    before, after = halo(1), halo(0)
    per = 2 * len(GROUPS)
    for p in range(BROWS // 2):
        window = jnp.where(across < 112, pair(p, 0), jnp.concatenate(before[per * p : per * (p + 1)], axis=0))
        resample(p, 0, window * scale[p])
        window = jnp.where(across < 16, jnp.concatenate(after[per * p : per * (p + 1)], axis=0), pair(p, 1))
        resample(p, 2, window * scale[p])

    for_neighbours(SIDES, lambda offset: copies[offset].wait_send())


def solution(mesh):
    n_xl, n_ta = mesh.shape["xl"], mesh.shape["ta"]
    table = filter_table()
    f32 = jnp.float32

    def shards(traces, steps):
        return pl.pallas_call(
            functools.partial(kernel, n_xl, n_ta),
            name="stack_resample",
            out_shape=jax.ShapeDtypeStruct((BROWS, BCOLS, OUT), f32),
            in_specs=[pl.BlockSpec(memory_space=pltpu.HBM)] * 3,
            out_specs=pl.BlockSpec(memory_space=pltpu.VMEM),
            scratch_shapes=[
                pltpu.VMEM((ROWS, COLS, SPAN), f32),
                pltpu.VMEM((2, ROWS, COLS), jnp.int32),
                pltpu.VMEM((2, ROWS, SPAN), jnp.int32),
                pltpu.VMEM((3, SPAN, SPAN), jnp.bfloat16),
                pltpu.VMEM((BROWS, 2, 3 * HALF, SPAN), jnp.bfloat16),
                pltpu.VMEM((BROWS + 2, 2 * HALF, OUT), f32),
                pltpu.VMEM((BROWS // 2, 2 * BCOLS, LANES), f32),
                pltpu.VMEM((2, BROWS, OUT), f32),
                pltpu.VMEM((2, 1, OUT), f32),
                pltpu.VMEM((2, BROWS, 8, LANES), f32),
                pltpu.VMEM((2, 8, LANES), f32),
                pltpu.VMEM((LAST_BIN + 1, OUT), f32),
                pltpu.VMEM((2, BROWS, OUT), f32),
                pltpu.VMEM((2, 1, OUT), f32),
                pltpu.VMEM((2, BROWS, 8, LANES), f32),
                pltpu.VMEM((2, 8, LANES), f32),
                pltpu.VMEM((2, 2, BROWS, LANES), f32),
                pltpu.VMEM((2, 2, 1, LANES), f32),
                pltpu.SemaphoreType.DMA((BROWS + 2,)),
                pltpu.SemaphoreType.DMA((len(OFFSETS),)),
                pltpu.SemaphoreType.DMA((len(OFFSETS),)),
            ],
            compiler_params=pltpu.CompilerParams(
                collective_id=0, has_side_effects=True, vmem_limit_bytes=32 * 1024 * 1024
            ),
        )(*(pltpu.with_memory_space_constraint(a, pltpu.HBM) for a in (traces, steps, jnp.asarray(table))))

    return jax.shard_map(
        shards,
        mesh=mesh,
        in_specs=(P("il", "xl", "ta"), P(None, "il", "xl")),
        out_specs=P("il", "xl", "ta"),
        check_vma=False,
    )
```

```python
import functools

import jax
import jax.numpy as jnp
import numpy as np
from jax import lax
from jax.experimental import pallas as pl
from jax.experimental.pallas import tpu as pltpu
from jax.sharding import PartitionSpec as P

TAPS = 16
P_SIZE = 3
Q = 2
REACH = TAPS // 2

LANES = 128
ROWS, COLS, SPAN = 16, 208, 256
BROWS, BCOLS, OUT = 8, 104, 384
HALVES = (64, 48)
STARTS = (0, 64)
HELD = 112
SPLIT = 56
FIRST_BIN, LAST_BIN = 0, 111
WINDOWS = ((0, 120), (104, 208))
GROUPS = tuple(range(0, 56, 8)) + tuple(range(64, 112, 8))

OFFSETS = tuple(
    (di, dx, dt) for di in (0, 1) for dx in (-1, 0, 1) for dt in (-1, 0, 1) if (di, dx, dt) != (0, 0, 0)
)


SIDES = ((-1, -1), (-1, 1), (1, -1), (1, 1), (0, -1), (0, 1), (-1, 0), (1, 0), (0, 0))
EARLY = SIDES[:4] + SIDES[6:8]
LATE = SIDES[4:6] + SIDES[8:]
BLOCKS = (range(0, 4), range(4, 8))


def filter_table():
    lane = np.arange(LANES)
    sample = np.stack(
        [
            np.where(lane < 112, lane, lane - 128),
            np.where(lane < 64, lane + 128, lane),
            np.where(lane < 16, lane + 256, lane + 128),
        ]
    )
    output = np.arange(OUT).reshape(3, LANES)
    x = (Q * output[:, None, :] - P_SIZE * sample[:, :, None]) / P_SIZE
    weights = np.where(np.abs(x) < REACH, np.sinc(x) * np.sinc(x / REACH), 0.0).astype(np.float32)
    high = weights.astype(jnp.bfloat16)
    low = (weights - high.astype(np.float32)).astype(jnp.bfloat16)
    top = np.concatenate([high, low], axis=2)
    bottom = np.concatenate([high, np.zeros_like(low)], axis=2)
    return np.concatenate([top, bottom], axis=1)


def halo_table():
    sample = np.arange(8)[:, None]
    weights = np.zeros((2, LANES, SPAN), np.float32)
    for end in (0, 1):
        n = sample - 8 if end else sample + SPAN
        x = (Q * (np.arange(16)[None, :] + (0 if end else OUT - 16)) - P_SIZE * n) / P_SIZE
        part = np.where(np.abs(x) < REACH, np.sinc(x) * np.sinc(x / REACH), 0.0)
        for r in range(len(GROUPS)):
            first = (8 * r + 120 * end) % LANES
            weights[end, first : first + 8, 16 * r : 16 * (r + 1)] = part
    high = weights.astype(jnp.bfloat16)
    low = (weights - high.astype(np.float32)).astype(jnp.bfloat16)
    return np.stack(
        [np.concatenate([high, high], axis=1), np.concatenate([low, np.zeros_like(low)], axis=1)], axis=1
    )


def parts_of(values):
    high = values.astype(jnp.bfloat16)
    low = (values - high.astype(jnp.float32)).astype(jnp.bfloat16)
    return high, low


def both(*conditions):
    held = [c for c in conditions if c is not None]
    return functools.reduce(jnp.logical_and, held) if held else None


def kernel(
    load_sem, send_sem, n_xl, n_ta, traces, steps, table, ends_table, out,
    x, edges, sv, cbuf, tab, tab_ends, onehot0, onehot1, acc, scale_packed, rims, packed, packed_rim,
    ra, rb, rc, rd, re, rf, rg, recv_sem,
):
    il, xl, ta = lax.axis_index("il"), lax.axis_index("xl"), lax.axis_index("ta")

    def there(step, index, size):
        return None if step == 0 else (index > 0 if step < 0 else index < size - 1)

    def device(offset):
        return {"il": 1 - il if offset[0] else il, "xl": xl + offset[1], "ta": ta + offset[2]}

    def for_neighbours(sides, action, sign=1):
        for dx, dt in sides:
            condition = both(there(sign * dx, xl, n_xl), there(sign * dt, ta, n_ta))

            def run(dx=dx, dt=dt):
                for di in (0, 1):
                    if (di, dx, dt) != (0, 0, 0):
                        action((di, dx, dt))

            if condition is None:
                run()
            else:
                pl.when(condition)(run)

    barrier = pltpu.get_barrier_semaphore()

    def greet(offset):
        pl.semaphore_signal(
            barrier, 1, device_id=device(offset), device_id_type=pl.DeviceIdType.MESH
        )

    for_neighbours(SIDES, greet)

    steps_copy = pltpu.make_async_copy(steps, sv, load_sem.at[0])
    steps_copy.start()
    edge_copies = []
    for side in (0, 1):
        columns = pl.ds((COLS - 8) * side, 8)
        edge_copies.append(pltpu.make_async_copy(traces.at[:, columns, :], edges.at[side], load_sem.at[1 + side]))
        edge_copies[-1].start()
    loads = []
    for block in BLOCKS:
        rows = pl.ds(2 * block[0], 2 * len(block))
        loads.append(pltpu.make_async_copy(traces.at[rows], x.at[rows], load_sem.at[3 + len(loads)]))
        loads[-1].start()
    table_copies = [
        pltpu.make_async_copy(table, tab, load_sem.at[3 + len(BLOCKS)]),
        pltpu.make_async_copy(ends_table, tab_ends, load_sem.at[4 + len(BLOCKS)]),
    ]
    for copy in table_copies:
        copy.start()

    edge = (1 - il) * (BROWS + 1)
    target = BROWS - (BROWS - 1) * il

    own, far = pl.ds(0, BROWS), pl.ds(BROWS, 1)
    copies = {}
    for number, offset in enumerate(OFFSETS):
        di, dx, dt = offset
        side, end = (dx + 1) // 2, (dt + 1) // 2
        lanes = pl.ds(LANES * end, LANES)
        if dt == 0 and dx == 0:
            source, place = acc.at[edge], ra
        elif dt == 0:
            source, place = (rims.at[side, far], rc.at[side]) if di else (rims.at[side, own], rb.at[side])
        elif dx == 0:
            source, place = (packed_rim.at[end], re.at[end]) if di else (packed.at[end], rd.at[end])
        elif di:
            source, place = rims.at[side, far, lanes], rg.at[end, side]
        else:
            source, place = rims.at[side, own, lanes], rf.at[end, side]
        copies[offset] = pltpu.make_async_remote_copy(
            src_ref=source,
            dst_ref=place,
            send_sem=send_sem.at[number],
            recv_sem=recv_sem.at[number],
            device_id=device(offset),
            device_id_type=pl.DeviceIdType.MESH,
        )

    for dx in (-1, 1):
        side = (dx + 1) // 2

        @pl.when(jnp.logical_not(there(-dx, xl, n_xl)))
        def _(side=side):
            for place in (rb.at[side], rc.at[side], *(r.at[e, side] for r in (rf, rg) for e in (0, 1))):
                place[...] = jnp.zeros(place.shape, jnp.float32)

    for dt in (-1, 1):
        end = (dt + 1) // 2

        @pl.when(jnp.logical_not(there(-dt, ta, n_ta)))
        def _(end=end):
            for place in (rd.at[end], re.at[end], rf.at[end], rg.at[end]):
                place[...] = jnp.zeros(place.shape, jnp.float32)

    steps_copy.wait()
    row_bin = lax.shift_right_logical(lax.broadcasted_iota(jnp.int32, (ROWS, COLS), 0), 1) + sv[0]
    inside = (row_bin >= 0) & (row_bin < BROWS)
    row_code = jnp.where(inside, row_bin, jnp.where(row_bin == edge - 1, BROWS, -1))
    wide = lax.broadcasted_iota(jnp.int32, (ROWS, SPAN), 1)
    bin_col = lax.shift_right_logical(lax.broadcasted_iota(jnp.int32, (ROWS, COLS), 1), 1) + sv[1]
    cbuf[...] = jnp.full(cbuf.shape, -1, jnp.int32)
    cbuf[0, :, 0:COLS] = jnp.where(
        (bin_col >= 0) & (bin_col < SPLIT), (sv[0] + 1) * HALVES[0] + bin_col, -1
    )
    cbuf[1, :, 0:COLS] = jnp.where(
        (bin_col >= SPLIT) & (bin_col < BCOLS), (sv[0] + 1) * HALVES[1] + bin_col - SPLIT, -1
    )
    first, second = cbuf[0], cbuf[1]
    codes = (
        (
            jnp.where(wide < 120, first, -1),
            jnp.where((wide >= 120) & (wide < 240), pltpu.roll(first, 120, 1), -1),
        ),
        (
            jnp.where(wide < 104, pltpu.roll(second, SPAN - 104, 1), -1),
            jnp.where((wide >= 104) & (wide < 208), second, -1),
        ),
    )
    onehot = (onehot0, onehot1)
    for h, size in enumerate(HALVES):
        places = lax.broadcasted_iota(jnp.int32, (3 * size, SPAN), 0)
        even, odd = codes[h]
        for k in range(BROWS):
            code = jnp.maximum(even[2 * k : 2 * k + 1], odd[2 * k + 1 : 2 * k + 2])
            onehot[h][k] = jnp.where(places == code, 1.0, 0.0).astype(jnp.bfloat16)

    for b in range(BROWS + 2):
        for h, size in enumerate(HALVES):
            rows = [onehot[h][k, size * (b - k) : size * (b - k + 1), :] for k in range(BROWS) if 0 <= b - k < 3]
            total = functools.reduce(jnp.add, rows)
            total = (total[:, :LANES] + total[:, LANES:]).astype(jnp.float32)
            acc[b, STARTS[h] : STARTS[h] + size, SPAN:OUT] = jnp.broadcast_to(
                jnp.sum(total, axis=1, keepdims=True), (size, LANES)
            )

    lane = lax.broadcasted_iota(jnp.int32, (8, LANES), 1)
    sublane = lax.broadcasted_iota(jnp.int32, (8, LANES), 0)

    def in_group(r, end):
        start = (8 * r + (120 if end else 0)) % LANES
        return (lane >= start) & (lane < start + 8)

    def pack(b, end):
        tile = pl.ds(LANES * end, LANES)
        total = acc[b, 0:8, tile]
        for r in range(1, len(GROUPS)):
            turned = pltpu.roll(acc[b, GROUPS[r] : GROUPS[r] + 8, tile], 8 * r, 1)
            total = jnp.where(in_group(r, end), turned, total)
        return total

    def send(offset):
        copies[offset].start()

    def find_rims():
        slots = lax.broadcasted_iota(jnp.int32, (ROWS, 2 * BROWS), 1)
        ones = jnp.ones((2 * ROWS, LANES), jnp.float32)
        for side in (0, 1):
            code = jnp.where(sv[1] == 2 * side - 1, row_code, -1)
            chosen, values = [], []
            for j in (0, 1):
                column = (COLS - 2) * side + j
                chosen.append(jnp.where(slots == code[:, column : column + 1], 1.0, 0.0))
                values.append(edges[side, :, 6 * side + j, :])
            rims[side] = lax.dot_general(
                jnp.concatenate(chosen, axis=0),
                jnp.concatenate([jnp.concatenate(values, axis=0), ones], axis=1),
                (((0,), (0,)), ((), ())),
                precision=lax.Precision.HIGHEST,
                preferred_element_type=jnp.float32,
            )

    distant = (lax.rem(ta, 4) == 0) | (ta == n_ta // 2 - 1)

    def meet():
        beside_xl = 1 + (xl > 0).astype(jnp.int32) + (xl < n_xl - 1).astype(jnp.int32)
        beside_ta = 1 + (ta > 0).astype(jnp.int32) + (ta < n_ta - 1).astype(jnp.int32)
        pl.semaphore_wait(barrier, 2 * beside_xl * beside_ta - 1)

    for block, load in zip(BLOCKS, loads):
        load.wait()
        if block is BLOCKS[0]:
            for copy in edge_copies:
                copy.wait()
            find_rims()
        for k in block:
            for h, size in enumerate(HALVES):
                start, stop = WINDOWS[h]
                pieces = [x[2 * k, start:stop, :], x[2 * k + 1, start:stop, :]]
                pieces.append(jnp.zeros((SPAN - 2 * (stop - start), SPAN), jnp.float32))
                high, low = parts_of(jnp.concatenate(pieces, axis=0))
                chosen = onehot[h][k]
                result = jnp.dot(chosen, high, preferred_element_type=jnp.float32)
                result = result + jnp.dot(chosen, low, preferred_element_type=jnp.float32)
                for q in range(3):
                    b = k + q
                    where = (b, pl.ds(STARTS[h], size), pl.ds(0, SPAN))
                    part = result[size * q : size * (q + 1)]
                    acc[where] = part if k == max(b - 2, 0) else acc[where] + part
            if k > 0:
                for end in (0, 1):
                    packed[end, k - 1] = pack(k, end)
        if block is BLOCKS[0]:

            @pl.when(jnp.logical_not(distant))
            def _():
                meet()
                for_neighbours(EARLY, send)

    for end in (0, 1):
        packed[end, BROWS - 1] = pack(BROWS, end)
        packed_rim[end] = pack(edge, end)

    @pl.when(distant)
    def _():
        meet()
        for_neighbours(EARLY, send)

    for_neighbours(LATE, send)

    for_neighbours(SIDES[6:], lambda offset: copies[offset].wait_recv(), -1)
    acc[target] = acc[target] + ra[...]
    for row, side in ((FIRST_BIN, 1), (LAST_BIN, 0)):
        acc[target, row : row + 1, :] = acc[target, row : row + 1, :] + rc[side]
        for b in range(BROWS):
            acc[b + 1, row : row + 1, :] = acc[b + 1, row : row + 1, :] + rb[side, b : b + 1, :]

    for copy in table_copies:
        copy.wait()

    def bins(b, tile):
        lanes = pl.ds(LANES * tile, LANES)
        return [acc[b, 0:SPLIT, lanes], acc[b, STARTS[1] : HELD, lanes]]

    def pair(p, tile):
        return jnp.concatenate(bins(2 * p + 1, tile) + bins(2 * p + 2, tile), axis=0)

    across = lax.broadcasted_iota(jnp.int32, (2 * BCOLS, LANES), 1)

    def resample(p, third, window):
        high, low = parts_of(window)
        result = jnp.dot(
            jnp.concatenate([high, low], axis=1), tab[third], preferred_element_type=jnp.float32
        )
        result = result[:, :LANES] + result[:, LANES:]
        lanes = pl.ds(LANES * third, LANES)
        out[2 * p, :, lanes] = result[:BCOLS]
        out[2 * p + 1, :, lanes] = result[BCOLS:]

    for p in range(BROWS // 2):
        factor = 1.0 / jnp.maximum(pair(p, 2), 1.0)
        low, high = pair(p, 0), pair(p, 1)
        resample(p, 1, jnp.where(across < 64, high, low) * factor)
        resample(p, 0, jnp.where(across < 112, low, 0.0) * factor)
        resample(p, 2, jnp.where(across < 16, 0.0, high) * factor)
        for b in (0, 1):
            for end in (0, 1):
                total = jnp.zeros((8, LANES), jnp.float32)
                for r in range(len(GROUPS)):
                    row = BCOLS * b + 8 * r
                    total = jnp.where(in_group(r, end), factor[row : row + 8], total)
                scale_packed[end, 2 * p + b] = total
    for_neighbours(SIDES, lambda offset: copies[offset].wait_send())

    for_neighbours(SIDES[:6], lambda offset: copies[offset].wait_recv(), -1)

    def halo(end):
        last = len(GROUPS) - 1
        here = in_group(0, end), in_group(last, end)
        near = [jnp.where(here[0], rf[end, 1], 0.0), jnp.where(here[1], pltpu.roll(rf[end, 0], 8 * last, 1), 0.0)]
        far = jnp.where(here[0] & (sublane == 0), rg[end, 1], 0.0)
        turned = pltpu.roll(jnp.broadcast_to(rg[end, 0], (8, LANES)), 8 * last, 1)
        far = far + jnp.where(here[1] & (sublane == 7), turned, 0.0) + re[end]
        rows = []
        for b in range(BROWS):
            tile = rd[end, b]
            tile = tile + jnp.where(sublane == 0, near[0][b : b + 1], 0.0)
            tile = tile + jnp.where(sublane == 7, near[1][b : b + 1], 0.0)
            if b in (0, BROWS - 1):
                tile = tile + jnp.where(target == b + 1, far, 0.0)
            rows.append(tile * scale_packed[end, b])
        high, low = parts_of(jnp.concatenate(rows, axis=0))
        halves = jnp.concatenate([high, low], axis=1)
        result = jnp.dot(halves, tab_ends[end, 0], preferred_element_type=jnp.float32)
        return result + jnp.dot(halves, tab_ends[end, 1], preferred_element_type=jnp.float32)

    before, after = halo(1), halo(0)
    for b in range(BROWS):
        for r in range(len(GROUPS)):
            tile = slice(LANES * (r // 8), LANES * (r // 8 + 1))
            start = 16 * (r % 8)
            rows = pl.ds(8 * r, 8)
            part = before[8 * b : 8 * (b + 1), tile]
            part = pltpu.roll(part, (LANES - start) % LANES, 1) if start else part
            lanes = pl.ds(0, LANES)
            out[b, rows, lanes] = out[b, rows, lanes] + jnp.where(lane < 16, part, 0.0)
            part = after[8 * b : 8 * (b + 1), tile]
            part = pltpu.roll(part, 112 - start, 1) if start < 112 else part
            lanes = pl.ds(2 * LANES, LANES)
            out[b, rows, lanes] = out[b, rows, lanes] + jnp.where(lane >= 112, part, 0.0)


def scoped(n_xl, n_ta, *refs):
    pl.run_scoped(
        lambda load_sem, send_sem: kernel(load_sem, send_sem, n_xl, n_ta, *refs),
        pltpu.SemaphoreType.DMA((5 + len(BLOCKS),)),
        pltpu.SemaphoreType.DMA((len(OFFSETS),)),
    )


def solution(mesh):
    n_xl, n_ta = mesh.shape["xl"], mesh.shape["ta"]
    tables = filter_table(), halo_table()
    f32 = jnp.float32

    def shards(traces, steps):
        return pl.pallas_call(
            functools.partial(scoped, n_xl, n_ta),
            name="stack_resample",
            out_shape=jax.ShapeDtypeStruct((BROWS, BCOLS, OUT), f32),
            in_specs=[pl.BlockSpec(memory_space=pltpu.HBM)] * 4,
            out_specs=pl.BlockSpec(memory_space=pltpu.VMEM),
            scratch_shapes=[
                pltpu.VMEM((ROWS, COLS, SPAN), f32),
                pltpu.VMEM((2, ROWS, 8, SPAN), f32),
                pltpu.VMEM((2, ROWS, COLS), jnp.int32),
                pltpu.VMEM((2, ROWS, SPAN), jnp.int32),
                pltpu.VMEM((3, SPAN, SPAN), jnp.bfloat16),
                pltpu.VMEM((2, 2, SPAN, SPAN), jnp.bfloat16),
                pltpu.VMEM((BROWS, 3 * HALVES[0], SPAN), jnp.bfloat16),
                pltpu.VMEM((BROWS, 3 * HALVES[1], SPAN), jnp.bfloat16),
                pltpu.VMEM((BROWS + 2, HELD, OUT), f32),
                pltpu.VMEM((2, BROWS, 8, LANES), f32),
                pltpu.VMEM((2, 2 * BROWS, OUT), f32),
                pltpu.VMEM((2, BROWS, 8, LANES), f32),
                pltpu.VMEM((2, 8, LANES), f32),
                pltpu.VMEM((HELD, OUT), f32),
                pltpu.VMEM((2, BROWS, OUT), f32),
                pltpu.VMEM((2, 1, OUT), f32),
                pltpu.VMEM((2, BROWS, 8, LANES), f32),
                pltpu.VMEM((2, 8, LANES), f32),
                pltpu.VMEM((2, 2, BROWS, LANES), f32),
                pltpu.VMEM((2, 2, 1, LANES), f32),
                pltpu.SemaphoreType.DMA((len(OFFSETS),)),
            ],
            compiler_params=pltpu.CompilerParams(
                collective_id=0, has_side_effects=True, vmem_limit_bytes=32 * 1024 * 1024
            ),
        )(*(pltpu.with_memory_space_constraint(a, pltpu.HBM) for a in (traces, steps, *map(jnp.asarray, tables))))

    return jax.shard_map(
        shards,
        mesh=mesh,
        in_specs=(P("il", "xl", "ta"), P(None, "il", "xl")),
        out_specs=P("il", "xl", "ta"),
        check_vma=False,
    )
```

```python
import functools

import jax
import jax.numpy as jnp
import numpy as np
from jax import lax
from jax.experimental import pallas as pl
from jax.experimental.pallas import tpu as pltpu
from jax.sharding import PartitionSpec as P

TAPS = 16
P_SIZE = 3
Q = 2
REACH = TAPS // 2

LANES = 128
ROWS, COLS, SPAN = 16, 208, 256
BROWS, BCOLS, OUT = 8, 104, 384
HALVES = (64, 48)
STARTS = (0, 64)
HELD = 112
SPLIT = 56
FIRST_BIN, LAST_BIN = 0, 111
WINDOWS = ((0, 120), (104, 208))
GROUPS = tuple(range(0, 56, 8)) + tuple(range(64, 112, 8))

OFFSETS = tuple(
    (di, dx, dt) for di in (0, 1) for dx in (-1, 0, 1) for dt in (-1, 0, 1) if (di, dx, dt) != (0, 0, 0)
)


SIDES = ((-1, -1), (-1, 1), (1, -1), (1, 1), (0, -1), (0, 1), (-1, 0), (1, 0), (0, 0))
EARLY = SIDES[:4] + SIDES[6:8]
LATE = SIDES[4:6] + SIDES[8:]
BLOCKS = (range(0, 4), range(4, 8))


def filter_table():
    lane = np.arange(LANES)
    sample = np.stack(
        [
            np.where(lane < 112, lane, lane - 128),
            np.where(lane < 64, lane + 128, lane),
            np.where(lane < 16, lane + 256, lane + 128),
        ]
    )
    output = np.arange(OUT).reshape(3, LANES)
    x = (Q * output[:, None, :] - P_SIZE * sample[:, :, None]) / P_SIZE
    weights = np.where(np.abs(x) < REACH, np.sinc(x) * np.sinc(x / REACH), 0.0).astype(np.float32)
    high = weights.astype(jnp.bfloat16)
    low = (weights - high.astype(np.float32)).astype(jnp.bfloat16)
    top = np.concatenate([high, low], axis=2)
    bottom = np.concatenate([high, np.zeros_like(low)], axis=2)
    return np.concatenate([top, bottom], axis=1)


def halo_table():
    sample = np.arange(8)[:, None]
    weights = np.zeros((2, LANES, SPAN), np.float32)
    for end in (0, 1):
        n = sample - 8 if end else sample + SPAN
        x = (Q * (np.arange(16)[None, :] + (0 if end else OUT - 16)) - P_SIZE * n) / P_SIZE
        part = np.where(np.abs(x) < REACH, np.sinc(x) * np.sinc(x / REACH), 0.0)
        for r in range(len(GROUPS)):
            first = (8 * r + 120 * end) % LANES
            weights[end, first : first + 8, 16 * r : 16 * (r + 1)] = part
    high = weights.astype(jnp.bfloat16)
    low = (weights - high.astype(np.float32)).astype(jnp.bfloat16)
    return np.stack(
        [np.concatenate([high, high], axis=1), np.concatenate([low, np.zeros_like(low)], axis=1)], axis=1
    )


def parts_of(values):
    high = values.astype(jnp.bfloat16)
    low = (values - high.astype(jnp.float32)).astype(jnp.bfloat16)
    return high, low


def both(*conditions):
    held = [c for c in conditions if c is not None]
    return functools.reduce(jnp.logical_and, held) if held else None


def kernel(
    load_sem, send_sem, n_xl, n_ta, traces, steps, table, ends_table, out, fixes,
    x, edges, sv, cbuf, tab, tab_ends, onehot0, onehot1, acc, scale_packed, rims, packed, packed_rim,
    ra, rb, rc, rd, re, rf, rg, recv_sem,
):
    il, xl, ta = lax.axis_index("il"), lax.axis_index("xl"), lax.axis_index("ta")

    def there(step, index, size):
        return None if step == 0 else (index > 0 if step < 0 else index < size - 1)

    def device(offset):
        return {"il": 1 - il if offset[0] else il, "xl": xl + offset[1], "ta": ta + offset[2]}

    def for_neighbours(sides, action, sign=1):
        for dx, dt in sides:
            condition = both(there(sign * dx, xl, n_xl), there(sign * dt, ta, n_ta))

            def run(dx=dx, dt=dt):
                for di in (0, 1):
                    if (di, dx, dt) != (0, 0, 0):
                        action((di, dx, dt))

            if condition is None:
                run()
            else:
                pl.when(condition)(run)

    barrier = pltpu.get_barrier_semaphore()

    def greet(offset):
        pl.semaphore_signal(
            barrier, 1, device_id=device(offset), device_id_type=pl.DeviceIdType.MESH
        )

    for_neighbours(SIDES, greet)

    steps_copy = pltpu.make_async_copy(steps, sv, load_sem.at[0])
    steps_copy.start()
    edge_copies = []
    for side in (0, 1):
        columns = pl.ds((COLS - 8) * side, 8)
        edge_copies.append(pltpu.make_async_copy(traces.at[:, columns, :], edges.at[side], load_sem.at[1 + side]))
        edge_copies[-1].start()
    loads = []
    for block in BLOCKS:
        rows = pl.ds(2 * block[0], 2 * len(block))
        loads.append(pltpu.make_async_copy(traces.at[rows], x.at[rows], load_sem.at[3 + len(loads)]))
        loads[-1].start()
    table_copies = [
        pltpu.make_async_copy(table, tab, load_sem.at[3 + len(BLOCKS)]),
        pltpu.make_async_copy(ends_table, tab_ends, load_sem.at[4 + len(BLOCKS)]),
    ]
    for copy in table_copies:
        copy.start()

    edge = (1 - il) * (BROWS + 1)
    target = BROWS - (BROWS - 1) * il

    own, far = pl.ds(0, BROWS), pl.ds(BROWS, 1)
    copies = {}
    for number, offset in enumerate(OFFSETS):
        di, dx, dt = offset
        side, end = (dx + 1) // 2, (dt + 1) // 2
        lanes = pl.ds(LANES * end, LANES)
        if dt == 0 and dx == 0:
            source, place = acc.at[edge], ra
        elif dt == 0:
            source, place = (rims.at[side, far], rc.at[side]) if di else (rims.at[side, own], rb.at[side])
        elif dx == 0:
            source, place = (packed_rim.at[end], re.at[end]) if di else (packed.at[end], rd.at[end])
        elif di:
            source, place = rims.at[side, far, lanes], rg.at[end, side]
        else:
            source, place = rims.at[side, own, lanes], rf.at[end, side]
        copies[offset] = pltpu.make_async_remote_copy(
            src_ref=source,
            dst_ref=place,
            send_sem=send_sem.at[number],
            recv_sem=recv_sem.at[number],
            device_id=device(offset),
            device_id_type=pl.DeviceIdType.MESH,
        )

    for dx in (-1, 1):
        side = (dx + 1) // 2

        @pl.when(jnp.logical_not(there(-dx, xl, n_xl)))
        def _(side=side):
            for place in (rb.at[side], rc.at[side], *(r.at[e, side] for r in (rf, rg) for e in (0, 1))):
                place[...] = jnp.zeros(place.shape, jnp.float32)

    for dt in (-1, 1):
        end = (dt + 1) // 2

        @pl.when(jnp.logical_not(there(-dt, ta, n_ta)))
        def _(end=end):
            for place in (rd.at[end], re.at[end], rf.at[end], rg.at[end]):
                place[...] = jnp.zeros(place.shape, jnp.float32)

    steps_copy.wait()
    row_bin = lax.shift_right_logical(lax.broadcasted_iota(jnp.int32, (ROWS, COLS), 0), 1) + sv[0]
    inside = (row_bin >= 0) & (row_bin < BROWS)
    row_code = jnp.where(inside, row_bin, jnp.where(row_bin == edge - 1, BROWS, -1))
    wide = lax.broadcasted_iota(jnp.int32, (ROWS, SPAN), 1)
    bin_col = lax.shift_right_logical(lax.broadcasted_iota(jnp.int32, (ROWS, COLS), 1), 1) + sv[1]
    cbuf[...] = jnp.full(cbuf.shape, -1, jnp.int32)
    cbuf[0, :, 0:COLS] = jnp.where(
        (bin_col >= 0) & (bin_col < SPLIT), (sv[0] + 1) * HALVES[0] + bin_col, -1
    )
    cbuf[1, :, 0:COLS] = jnp.where(
        (bin_col >= SPLIT) & (bin_col < BCOLS), (sv[0] + 1) * HALVES[1] + bin_col - SPLIT, -1
    )
    first, second = cbuf[0], cbuf[1]
    codes = (
        (
            jnp.where(wide < 120, first, -1),
            jnp.where((wide >= 120) & (wide < 240), pltpu.roll(first, 120, 1), -1),
        ),
        (
            jnp.where(wide < 104, pltpu.roll(second, SPAN - 104, 1), -1),
            jnp.where((wide >= 104) & (wide < 208), second, -1),
        ),
    )
    onehot = (onehot0, onehot1)
    for h, size in enumerate(HALVES):
        places = lax.broadcasted_iota(jnp.int32, (3 * size, SPAN), 0)
        even, odd = codes[h]
        for k in range(BROWS):
            code = jnp.maximum(even[2 * k : 2 * k + 1], odd[2 * k + 1 : 2 * k + 2])
            onehot[h][k] = jnp.where(places == code, 1.0, 0.0).astype(jnp.bfloat16)

    for b in range(BROWS + 2):
        for h, size in enumerate(HALVES):
            rows = [onehot[h][k, size * (b - k) : size * (b - k + 1), :] for k in range(BROWS) if 0 <= b - k < 3]
            total = functools.reduce(jnp.add, rows)
            total = (total[:, :LANES] + total[:, LANES:]).astype(jnp.float32)
            acc[b, STARTS[h] : STARTS[h] + size, SPAN:OUT] = jnp.broadcast_to(
                jnp.sum(total, axis=1, keepdims=True), (size, LANES)
            )

    lane = lax.broadcasted_iota(jnp.int32, (8, LANES), 1)
    sublane = lax.broadcasted_iota(jnp.int32, (8, LANES), 0)

    def in_group(r, end):
        start = (8 * r + (120 if end else 0)) % LANES
        return (lane >= start) & (lane < start + 8)

    def pack(b, end):
        tile = pl.ds(LANES * end, LANES)
        total = acc[b, 0:8, tile]
        for r in range(1, len(GROUPS)):
            turned = pltpu.roll(acc[b, GROUPS[r] : GROUPS[r] + 8, tile], 8 * r, 1)
            total = jnp.where(in_group(r, end), turned, total)
        return total

    def send(offset):
        copies[offset].start()

    def find_rims():
        slots = lax.broadcasted_iota(jnp.int32, (ROWS, 2 * BROWS), 1)
        ones = jnp.ones((2 * ROWS, LANES), jnp.float32)
        for side in (0, 1):
            code = jnp.where(sv[1] == 2 * side - 1, row_code, -1)
            chosen, values = [], []
            for j in (0, 1):
                column = (COLS - 2) * side + j
                chosen.append(jnp.where(slots == code[:, column : column + 1], 1.0, 0.0))
                values.append(edges[side, :, 6 * side + j, :])
            rims[side] = lax.dot_general(
                jnp.concatenate(chosen, axis=0),
                jnp.concatenate([jnp.concatenate(values, axis=0), ones], axis=1),
                (((0,), (0,)), ((), ())),
                precision=lax.Precision.HIGHEST,
                preferred_element_type=jnp.float32,
            )

    distant = (lax.rem(ta, 4) == 0) | (ta == n_ta // 2 - 1)

    def meet():
        beside_xl = 1 + (xl > 0).astype(jnp.int32) + (xl < n_xl - 1).astype(jnp.int32)
        beside_ta = 1 + (ta > 0).astype(jnp.int32) + (ta < n_ta - 1).astype(jnp.int32)
        pl.semaphore_wait(barrier, 2 * beside_xl * beside_ta - 1)

    for block, load in zip(BLOCKS, loads):
        load.wait()
        if block is BLOCKS[0]:
            for copy in edge_copies:
                copy.wait()
            find_rims()
        for k in block:
            for h, size in enumerate(HALVES):
                start, stop = WINDOWS[h]
                pieces = [x[2 * k, start:stop, :], x[2 * k + 1, start:stop, :]]
                pieces.append(jnp.zeros((SPAN - 2 * (stop - start), SPAN), jnp.float32))
                high, low = parts_of(jnp.concatenate(pieces, axis=0))
                chosen = onehot[h][k]
                result = jnp.dot(chosen, high, preferred_element_type=jnp.float32)
                result = result + jnp.dot(chosen, low, preferred_element_type=jnp.float32)
                for q in range(3):
                    b = k + q
                    where = (b, pl.ds(STARTS[h], size), pl.ds(0, SPAN))
                    part = result[size * q : size * (q + 1)]
                    acc[where] = part if k == max(b - 2, 0) else acc[where] + part
            if k > 0:
                for end in (0, 1):
                    packed[end, k - 1] = pack(k, end)
        if block is BLOCKS[0]:

            @pl.when(jnp.logical_not(distant))
            def _():
                meet()
                for_neighbours(EARLY, send)

    for end in (0, 1):
        packed[end, BROWS - 1] = pack(BROWS, end)
        packed_rim[end] = pack(edge, end)

    @pl.when(distant)
    def _():
        meet()
        for_neighbours(EARLY, send)

    for_neighbours(LATE, send)

    for_neighbours(SIDES[6:], lambda offset: copies[offset].wait_recv(), -1)
    acc[target] = acc[target] + ra[...]
    for row, side in ((FIRST_BIN, 1), (LAST_BIN, 0)):
        acc[target, row : row + 1, :] = acc[target, row : row + 1, :] + rc[side]
        for b in range(BROWS):
            acc[b + 1, row : row + 1, :] = acc[b + 1, row : row + 1, :] + rb[side, b : b + 1, :]

    for copy in table_copies:
        copy.wait()

    def bins(b, tile):
        lanes = pl.ds(LANES * tile, LANES)
        return [acc[b, 0:SPLIT, lanes], acc[b, STARTS[1] : HELD, lanes]]

    def pair(p, tile):
        return jnp.concatenate(bins(2 * p + 1, tile) + bins(2 * p + 2, tile), axis=0)

    across = lax.broadcasted_iota(jnp.int32, (2 * BCOLS, LANES), 1)

    def resample(p, third, window):
        high, low = parts_of(window)
        result = jnp.dot(
            jnp.concatenate([high, low], axis=1), tab[third], preferred_element_type=jnp.float32
        )
        result = result[:, :LANES] + result[:, LANES:]
        lanes = pl.ds(LANES * third, LANES)
        out[2 * p, :, lanes] = result[:BCOLS]
        out[2 * p + 1, :, lanes] = result[BCOLS:]

    for p in range(BROWS // 2):
        factor = 1.0 / jnp.maximum(pair(p, 2), 1.0)
        low, high = pair(p, 0), pair(p, 1)
        resample(p, 1, jnp.where(across < 64, high, low) * factor)
        resample(p, 0, jnp.where(across < 112, low, 0.0) * factor)
        resample(p, 2, jnp.where(across < 16, 0.0, high) * factor)
        for b in (0, 1):
            for end in (0, 1):
                total = jnp.zeros((8, LANES), jnp.float32)
                for r in range(len(GROUPS)):
                    row = BCOLS * b + 8 * r
                    total = jnp.where(in_group(r, end), factor[row : row + 8], total)
                scale_packed[end, 2 * p + b] = total
    for_neighbours(SIDES, lambda offset: copies[offset].wait_send())

    for_neighbours(SIDES[:6], lambda offset: copies[offset].wait_recv(), -1)

    def halo(end):
        last = len(GROUPS) - 1
        here = in_group(0, end), in_group(last, end)
        near = [jnp.where(here[0], rf[end, 1], 0.0), jnp.where(here[1], pltpu.roll(rf[end, 0], 8 * last, 1), 0.0)]
        far = jnp.where(here[0] & (sublane == 0), rg[end, 1], 0.0)
        turned = pltpu.roll(jnp.broadcast_to(rg[end, 0], (8, LANES)), 8 * last, 1)
        far = far + jnp.where(here[1] & (sublane == 7), turned, 0.0) + re[end]
        rows = []
        for b in range(BROWS):
            tile = rd[end, b]
            tile = tile + jnp.where(sublane == 0, near[0][b : b + 1], 0.0)
            tile = tile + jnp.where(sublane == 7, near[1][b : b + 1], 0.0)
            if b in (0, BROWS - 1):
                tile = tile + jnp.where(target == b + 1, far, 0.0)
            rows.append(tile * scale_packed[end, b])
        high, low = parts_of(jnp.concatenate(rows, axis=0))
        halves = jnp.concatenate([high, low], axis=1)
        result = jnp.dot(halves, tab_ends[end, 0], preferred_element_type=jnp.float32)
        return result + jnp.dot(halves, tab_ends[end, 1], preferred_element_type=jnp.float32)

    for end in (0, 1):
        fixes[end] = halo(end)


def finish(sems, own, fixes, out, ends):
    middle = pl.ds(LANES, LANES)
    copies = [pltpu.make_async_copy(own.at[:, :, middle], out.at[:, :, middle], sems.at[0])]
    copies[0].start()
    lane = lax.broadcasted_iota(jnp.int32, (8, LANES), 1)
    for p in range(BROWS // 2):
        for b in (2 * p, 2 * p + 1):
            for r in range(len(GROUPS)):
                tile = slice(LANES * (r // 8), LANES * (r // 8 + 1))
                start = 16 * (r % 8)
                rows = pl.ds(8 * r, 8)
                part = fixes[1, 8 * b : 8 * (b + 1), tile]
                part = pltpu.roll(part, (LANES - start) % LANES, 1) if start else part
                ends[1, b, rows, :] = own[b, rows, 0:LANES] + jnp.where(lane < 16, part, 0.0)
                part = fixes[0, 8 * b : 8 * (b + 1), tile]
                part = pltpu.roll(part, 112 - start, 1) if start < 112 else part
                ends[0, b, rows, :] = own[b, rows, 2 * LANES : OUT] + jnp.where(lane >= 112, part, 0.0)
        for end in (0, 1):
            bs = pl.ds(2 * p, 2)
            lanes = pl.ds(0 if end else 2 * LANES, LANES)
            copies.append(pltpu.make_async_copy(ends.at[end, bs], out.at[bs, :, lanes], sems.at[len(copies)]))
            copies[-1].start()
    for copy in copies:
        copy.wait()


def scoped(n_xl, n_ta, *refs):
    pl.run_scoped(
        lambda load_sem, send_sem: kernel(load_sem, send_sem, n_xl, n_ta, *refs),
        pltpu.SemaphoreType.DMA((5 + len(BLOCKS),)),
        pltpu.SemaphoreType.DMA((len(OFFSETS),)),
    )


def solution(mesh):
    n_xl, n_ta = mesh.shape["xl"], mesh.shape["ta"]
    tables = filter_table(), halo_table()
    f32 = jnp.float32

    def shards(traces, steps):
        own, fixes = pl.pallas_call(
            functools.partial(scoped, n_xl, n_ta),
            name="stack_resample",
            out_shape=(
                jax.ShapeDtypeStruct((BROWS, BCOLS, OUT), f32),
                jax.ShapeDtypeStruct((2, 8 * BROWS, SPAN), f32),
            ),
            in_specs=[pl.BlockSpec(memory_space=pltpu.HBM)] * 4,
            out_specs=(pl.BlockSpec(memory_space=pltpu.VMEM),) * 2,
            scratch_shapes=[
                pltpu.VMEM((ROWS, COLS, SPAN), f32),
                pltpu.VMEM((2, ROWS, 8, SPAN), f32),
                pltpu.VMEM((2, ROWS, COLS), jnp.int32),
                pltpu.VMEM((2, ROWS, SPAN), jnp.int32),
                pltpu.VMEM((3, SPAN, SPAN), jnp.bfloat16),
                pltpu.VMEM((2, 2, SPAN, SPAN), jnp.bfloat16),
                pltpu.VMEM((BROWS, 3 * HALVES[0], SPAN), jnp.bfloat16),
                pltpu.VMEM((BROWS, 3 * HALVES[1], SPAN), jnp.bfloat16),
                pltpu.VMEM((BROWS + 2, HELD, OUT), f32),
                pltpu.VMEM((2, BROWS, 8, LANES), f32),
                pltpu.VMEM((2, 2 * BROWS, OUT), f32),
                pltpu.VMEM((2, BROWS, 8, LANES), f32),
                pltpu.VMEM((2, 8, LANES), f32),
                pltpu.VMEM((HELD, OUT), f32),
                pltpu.VMEM((2, BROWS, OUT), f32),
                pltpu.VMEM((2, 1, OUT), f32),
                pltpu.VMEM((2, BROWS, 8, LANES), f32),
                pltpu.VMEM((2, 8, LANES), f32),
                pltpu.VMEM((2, 2, BROWS, LANES), f32),
                pltpu.VMEM((2, 2, 1, LANES), f32),
                pltpu.SemaphoreType.DMA((len(OFFSETS),)),
            ],
            compiler_params=pltpu.CompilerParams(
                collective_id=0, has_side_effects=True, vmem_limit_bytes=32 * 1024 * 1024
            ),
        )(*(pltpu.with_memory_space_constraint(a, pltpu.HBM) for a in (traces, steps, *map(jnp.asarray, tables))))
        return pl.pallas_call(
            lambda *refs: pl.run_scoped(
                lambda sems: finish(sems, *refs), pltpu.SemaphoreType.DMA((1 + BROWS,))
            ),
            name="finish",
            out_shape=jax.ShapeDtypeStruct((BROWS, BCOLS, OUT), f32),
            in_specs=[pl.BlockSpec(memory_space=pltpu.VMEM)] * 2,
            out_specs=pl.BlockSpec(memory_space=pltpu.HBM),
            scratch_shapes=[
                pltpu.VMEM((2, BROWS, BCOLS, LANES), f32),
            ],
            compiler_params=pltpu.CompilerParams(vmem_limit_bytes=16 * 1024 * 1024),
        )(own, fixes)

    return jax.shard_map(
        shards,
        mesh=mesh,
        in_specs=(P("il", "xl", "ta"), P(None, "il", "xl")),
        out_specs=P("il", "xl", "ta"),
        check_vma=False,
    )
```

```python
import functools

import jax
import jax.numpy as jnp
import numpy as np
from jax import lax
from jax.experimental import pallas as pl
from jax.experimental.pallas import tpu as pltpu
from jax.sharding import PartitionSpec as P

TAPS = 16
P_SIZE = 3
Q = 2
REACH = TAPS // 2

LANES = 128
ROWS, COLS, SPAN = 16, 208, 256
BROWS, BCOLS, OUT = 8, 104, 384
HALVES = (64, 48)
STARTS = (0, 64)
HELD = 112
SPLIT = 56
FIRST_BIN, LAST_BIN = 0, 111
WINDOWS = ((0, 120), (104, 208))
GROUPS = tuple(range(0, 56, 8)) + tuple(range(64, 112, 8))

OFFSETS = tuple(
    (di, dx, dt) for di in (0, 1) for dx in (-1, 0, 1) for dt in (-1, 0, 1) if (di, dx, dt) != (0, 0, 0)
)


SIDES = ((-1, -1), (-1, 1), (1, -1), (1, 1), (0, -1), (0, 1), (-1, 0), (1, 0), (0, 0))
EARLY = SIDES[:4] + SIDES[6:8]
LATE = SIDES[4:6] + SIDES[8:]
BLOCKS = (range(0, 3), range(3, 8))


def filter_table():
    lane = np.arange(LANES)
    sample = np.stack(
        [
            np.where(lane < 112, lane, lane - 128),
            np.where(lane < 64, lane + 128, lane),
            np.where(lane < 16, lane + 256, lane + 128),
        ]
    )
    output = np.arange(OUT).reshape(3, LANES)
    x = (Q * output[:, None, :] - P_SIZE * sample[:, :, None]) / P_SIZE
    weights = np.where(np.abs(x) < REACH, np.sinc(x) * np.sinc(x / REACH), 0.0).astype(np.float32)
    high = weights.astype(jnp.bfloat16)
    low = (weights - high.astype(np.float32)).astype(jnp.bfloat16)
    top = np.concatenate([high, low], axis=2)
    bottom = np.concatenate([high, np.zeros_like(low)], axis=2)
    return np.concatenate([top, bottom], axis=1)


def halo_table():
    sample = np.arange(8)[:, None]
    weights = np.zeros((2, LANES, SPAN), np.float32)
    for end in (0, 1):
        n = sample - 8 if end else sample + SPAN
        x = (Q * (np.arange(16)[None, :] + (0 if end else OUT - 16)) - P_SIZE * n) / P_SIZE
        part = np.where(np.abs(x) < REACH, np.sinc(x) * np.sinc(x / REACH), 0.0)
        for r in range(len(GROUPS)):
            first = (8 * r + 120 * end) % LANES
            weights[end, first : first + 8, 16 * r : 16 * (r + 1)] = part
    high = weights.astype(jnp.bfloat16)
    low = (weights - high.astype(np.float32)).astype(jnp.bfloat16)
    return np.stack(
        [np.concatenate([high, high], axis=1), np.concatenate([low, np.zeros_like(low)], axis=1)], axis=1
    )


def in_group(r, end):
    start = (8 * r + (120 if end else 0)) % LANES
    lane = lax.broadcasted_iota(jnp.int32, (8, LANES), 1)
    return (lane >= start) & (lane < start + 8)


def parts_of(values):
    high = values.astype(jnp.bfloat16)
    low = (values - high.astype(jnp.float32)).astype(jnp.bfloat16)
    return high, low


def both(*conditions):
    held = [c for c in conditions if c is not None]
    return functools.reduce(jnp.logical_and, held) if held else None


def kernel(
    load_sem, send_sem, n_xl, n_ta, traces, steps, table, ends_table, out, tab_ends, scale_packed, rd, re, rf, rg,
    x, edges, sv, cbuf, tab, onehot0, onehot1, acc, rims, packed, packed_rim,
    ra, rb, rc, recv_sem,
):
    il, xl, ta = lax.axis_index("il"), lax.axis_index("xl"), lax.axis_index("ta")

    def there(step, index, size):
        return None if step == 0 else (index > 0 if step < 0 else index < size - 1)

    def device(offset):
        return {"il": 1 - il if offset[0] else il, "xl": xl + offset[1], "ta": ta + offset[2]}

    def for_neighbours(sides, action, sign=1):
        for dx, dt in sides:
            condition = both(there(sign * dx, xl, n_xl), there(sign * dt, ta, n_ta))

            def run(dx=dx, dt=dt):
                for di in (0, 1):
                    if (di, dx, dt) != (0, 0, 0):
                        action((di, dx, dt))

            if condition is None:
                run()
            else:
                pl.when(condition)(run)

    barrier = pltpu.get_barrier_semaphore()

    def greet(offset):
        pl.semaphore_signal(
            barrier, 1, device_id=device(offset), device_id_type=pl.DeviceIdType.MESH
        )

    for_neighbours(SIDES, greet)

    steps_copy = pltpu.make_async_copy(steps, sv, load_sem.at[0])
    steps_copy.start()
    edge_copies = []
    for side in (0, 1):
        columns = pl.ds((COLS - 8) * side, 8)
        edge_copies.append(pltpu.make_async_copy(traces.at[:, columns, :], edges.at[side], load_sem.at[1 + side]))
        edge_copies[-1].start()
    loads = []
    for block in BLOCKS:
        rows = pl.ds(2 * block[0], 2 * len(block))
        loads.append(pltpu.make_async_copy(traces.at[rows], x.at[rows], load_sem.at[3 + len(loads)]))
        loads[-1].start()
    table_copies = [
        pltpu.make_async_copy(table, tab, load_sem.at[3 + len(BLOCKS)]),
        pltpu.make_async_copy(ends_table, tab_ends, load_sem.at[4 + len(BLOCKS)]),
    ]
    for copy in table_copies:
        copy.start()

    edge = (1 - il) * (BROWS + 1)
    target = BROWS - (BROWS - 1) * il

    own, far = pl.ds(0, BROWS), pl.ds(BROWS, 1)
    copies = {}
    for number, offset in enumerate(OFFSETS):
        di, dx, dt = offset
        side, end = (dx + 1) // 2, (dt + 1) // 2
        lanes = pl.ds(LANES * end, LANES)
        if dt == 0 and dx == 0:
            source, place = acc.at[edge], ra
        elif dt == 0:
            source, place = (rims.at[side, far], rc.at[side]) if di else (rims.at[side, own], rb.at[side])
        elif dx == 0:
            source, place = (packed_rim.at[end], re.at[end]) if di else (packed.at[end], rd.at[end])
        elif di:
            source, place = rims.at[side, far, lanes], rg.at[end, side]
        else:
            source, place = rims.at[side, own, lanes], rf.at[end, side]
        copies[offset] = pltpu.make_async_remote_copy(
            src_ref=source,
            dst_ref=place,
            send_sem=send_sem.at[number],
            recv_sem=recv_sem.at[number],
            device_id=device(offset),
            device_id_type=pl.DeviceIdType.MESH,
        )

    for dx in (-1, 1):
        side = (dx + 1) // 2

        @pl.when(jnp.logical_not(there(-dx, xl, n_xl)))
        def _(side=side):
            for place in (rb.at[side], rc.at[side], *(r.at[e, side] for r in (rf, rg) for e in (0, 1))):
                place[...] = jnp.zeros(place.shape, jnp.float32)

    for dt in (-1, 1):
        end = (dt + 1) // 2

        @pl.when(jnp.logical_not(there(-dt, ta, n_ta)))
        def _(end=end):
            for place in (rd.at[end], re.at[end], rf.at[end], rg.at[end]):
                place[...] = jnp.zeros(place.shape, jnp.float32)

    steps_copy.wait()
    row_bin = lax.shift_right_logical(lax.broadcasted_iota(jnp.int32, (ROWS, COLS), 0), 1) + sv[0]
    inside = (row_bin >= 0) & (row_bin < BROWS)
    row_code = jnp.where(inside, row_bin, jnp.where(row_bin == edge - 1, BROWS, -1))
    wide = lax.broadcasted_iota(jnp.int32, (ROWS, SPAN), 1)
    bin_col = lax.shift_right_logical(lax.broadcasted_iota(jnp.int32, (ROWS, COLS), 1), 1) + sv[1]
    cbuf[...] = jnp.full(cbuf.shape, -1, jnp.int32)
    cbuf[0, :, 0:COLS] = jnp.where(
        (bin_col >= 0) & (bin_col < SPLIT), (sv[0] + 1) * HALVES[0] + bin_col, -1
    )
    cbuf[1, :, 0:COLS] = jnp.where(
        (bin_col >= SPLIT) & (bin_col < BCOLS), (sv[0] + 1) * HALVES[1] + bin_col - SPLIT, -1
    )
    first, second = cbuf[0], cbuf[1]
    codes = (
        (
            jnp.where(wide < 120, first, -1),
            jnp.where((wide >= 120) & (wide < 240), pltpu.roll(first, 120, 1), -1),
        ),
        (
            jnp.where(wide < 104, pltpu.roll(second, SPAN - 104, 1), -1),
            jnp.where((wide >= 104) & (wide < 208), second, -1),
        ),
    )
    onehot = (onehot0, onehot1)
    for h, size in enumerate(HALVES):
        places = lax.broadcasted_iota(jnp.int32, (3 * size, SPAN), 0)
        even, odd = codes[h]
        for k in range(BROWS):
            code = jnp.maximum(even[2 * k : 2 * k + 1], odd[2 * k + 1 : 2 * k + 2])
            onehot[h][k] = jnp.where(places == code, 1.0, 0.0).astype(jnp.bfloat16)

    for b in range(BROWS + 2):
        for h, size in enumerate(HALVES):
            rows = [onehot[h][k, size * (b - k) : size * (b - k + 1), :] for k in range(BROWS) if 0 <= b - k < 3]
            total = functools.reduce(jnp.add, rows)
            total = (total[:, :LANES] + total[:, LANES:]).astype(jnp.float32)
            acc[b, STARTS[h] : STARTS[h] + size, SPAN:OUT] = jnp.broadcast_to(
                jnp.sum(total, axis=1, keepdims=True), (size, LANES)
            )

    lane = lax.broadcasted_iota(jnp.int32, (8, LANES), 1)
    def pack(b, end):
        tile = pl.ds(LANES * end, LANES)
        total = acc[b, 0:8, tile]
        for r in range(1, len(GROUPS)):
            turned = pltpu.roll(acc[b, GROUPS[r] : GROUPS[r] + 8, tile], 8 * r, 1)
            total = jnp.where(in_group(r, end), turned, total)
        return total

    def send(offset):
        copies[offset].start()

    def find_rims():
        slots = lax.broadcasted_iota(jnp.int32, (ROWS, 2 * BROWS), 1)
        ones = jnp.ones((2 * ROWS, LANES), jnp.float32)
        for side in (0, 1):
            code = jnp.where(sv[1] == 2 * side - 1, row_code, -1)
            chosen, values = [], []
            for j in (0, 1):
                column = (COLS - 2) * side + j
                chosen.append(jnp.where(slots == code[:, column : column + 1], 1.0, 0.0))
                values.append(edges[side, :, 6 * side + j, :])
            rims[side] = lax.dot_general(
                jnp.concatenate(chosen, axis=0),
                jnp.concatenate([jnp.concatenate(values, axis=0), ones], axis=1),
                (((0,), (0,)), ((), ())),
                precision=lax.Precision.HIGHEST,
                preferred_element_type=jnp.float32,
            )

    distant = (lax.rem(ta, 4) == 0) | (ta == n_ta // 2 - 1)

    def meet():
        beside_xl = 1 + (xl > 0).astype(jnp.int32) + (xl < n_xl - 1).astype(jnp.int32)
        beside_ta = 1 + (ta > 0).astype(jnp.int32) + (ta < n_ta - 1).astype(jnp.int32)
        pl.semaphore_wait(barrier, 2 * beside_xl * beside_ta - 1)

    for block, load in zip(BLOCKS, loads):
        load.wait()
        if block is BLOCKS[0]:
            for copy in edge_copies:
                copy.wait()
            find_rims()
        for k in block:
            for h, size in enumerate(HALVES):
                start, stop = WINDOWS[h]
                pieces = [x[2 * k, start:stop, :], x[2 * k + 1, start:stop, :]]
                pieces.append(jnp.zeros((SPAN - 2 * (stop - start), SPAN), jnp.float32))
                high, low = parts_of(jnp.concatenate(pieces, axis=0))
                chosen = onehot[h][k]
                result = jnp.dot(chosen, high, preferred_element_type=jnp.float32)
                result = result + jnp.dot(chosen, low, preferred_element_type=jnp.float32)
                for q in range(3):
                    b = k + q
                    where = (b, pl.ds(STARTS[h], size), pl.ds(0, SPAN))
                    part = result[size * q : size * (q + 1)]
                    acc[where] = part if k == max(b - 2, 0) else acc[where] + part
            if k > 0:
                for end in (0, 1):
                    packed[end, k - 1] = pack(k, end)
        if block is BLOCKS[0]:

            @pl.when(jnp.logical_not(distant))
            def _():
                meet()
                for_neighbours(EARLY, send)

    for end in (0, 1):
        packed[end, BROWS - 1] = pack(BROWS, end)
        packed_rim[end] = pack(edge, end)

    @pl.when(distant)
    def _():
        meet()
        for_neighbours(EARLY, send)

    for_neighbours(LATE, send)

    for_neighbours(SIDES[6:], lambda offset: copies[offset].wait_recv(), -1)
    acc[target] = acc[target] + ra[...]
    for row, side in ((FIRST_BIN, 1), (LAST_BIN, 0)):
        acc[target, row : row + 1, :] = acc[target, row : row + 1, :] + rc[side]
        for b in range(BROWS):
            acc[b + 1, row : row + 1, :] = acc[b + 1, row : row + 1, :] + rb[side, b : b + 1, :]

    for copy in table_copies:
        copy.wait()

    def bins(b, tile):
        lanes = pl.ds(LANES * tile, LANES)
        return [acc[b, 0:SPLIT, lanes], acc[b, STARTS[1] : HELD, lanes]]

    def pair(p, tile):
        return jnp.concatenate(bins(2 * p + 1, tile) + bins(2 * p + 2, tile), axis=0)

    across = lax.broadcasted_iota(jnp.int32, (2 * BCOLS, LANES), 1)

    def resample(p, third, window):
        high, low = parts_of(window)
        result = jnp.dot(
            jnp.concatenate([high, low], axis=1), tab[third], preferred_element_type=jnp.float32
        )
        result = result[:, :LANES] + result[:, LANES:]
        lanes = pl.ds(LANES * third, LANES)
        out[2 * p, :, lanes] = result[:BCOLS]
        out[2 * p + 1, :, lanes] = result[BCOLS:]

    for p in range(BROWS // 2):
        factor = 1.0 / jnp.maximum(pair(p, 2), 1.0)
        low, high = pair(p, 0), pair(p, 1)
        resample(p, 1, jnp.where(across < 64, high, low) * factor)
        resample(p, 0, jnp.where(across < 112, low, 0.0) * factor)
        resample(p, 2, jnp.where(across < 16, 0.0, high) * factor)
        for b in (0, 1):
            for end in (0, 1):
                total = jnp.zeros((8, LANES), jnp.float32)
                for r in range(len(GROUPS)):
                    row = BCOLS * b + 8 * r
                    total = jnp.where(in_group(r, end), factor[row : row + 8], total)
                scale_packed[end, 2 * p + b] = total
    for_neighbours(SIDES, lambda offset: copies[offset].wait_send())

    for_neighbours(SIDES[:6], lambda offset: copies[offset].wait_recv(), -1)


def finish(sems, own, tab_ends, scale_packed, rd, re, rf, rg, out, ends):
    middle = pl.ds(LANES, LANES)
    copies = [pltpu.make_async_copy(own.at[:, :, middle], out.at[:, :, middle], sems.at[0])]
    copies[0].start()
    lane = lax.broadcasted_iota(jnp.int32, (8, LANES), 1)
    sublane = lax.broadcasted_iota(jnp.int32, (8, LANES), 0)
    target = BROWS - (BROWS - 1) * lax.axis_index("il")

    def halo(end):
        last = len(GROUPS) - 1
        here = in_group(0, end), in_group(last, end)
        near = [jnp.where(here[0], rf[end, 1], 0.0), jnp.where(here[1], pltpu.roll(rf[end, 0], 8 * last, 1), 0.0)]
        far = jnp.where(here[0] & (sublane == 0), rg[end, 1], 0.0)
        turned = pltpu.roll(jnp.broadcast_to(rg[end, 0], (8, LANES)), 8 * last, 1)
        far = far + jnp.where(here[1] & (sublane == 7), turned, 0.0) + re[end]
        rows = []
        for b in range(BROWS):
            tile = rd[end, b]
            tile = tile + jnp.where(sublane == 0, near[0][b : b + 1], 0.0)
            tile = tile + jnp.where(sublane == 7, near[1][b : b + 1], 0.0)
            if b in (0, BROWS - 1):
                tile = tile + jnp.where(target == b + 1, far, 0.0)
            rows.append(tile * scale_packed[end, b])
        high, low = parts_of(jnp.concatenate(rows, axis=0))
        halves = jnp.concatenate([high, low], axis=1)
        result = jnp.dot(halves, tab_ends[end, 0], preferred_element_type=jnp.float32)
        return result + jnp.dot(halves, tab_ends[end, 1], preferred_element_type=jnp.float32)

    fixes = halo(0), halo(1)
    for p in range(BROWS // 2):
        for b in (2 * p, 2 * p + 1):
            for r in range(len(GROUPS)):
                tile = slice(LANES * (r // 8), LANES * (r // 8 + 1))
                start = 16 * (r % 8)
                rows = pl.ds(8 * r, 8)
                part = fixes[1][8 * b : 8 * (b + 1), tile]
                part = pltpu.roll(part, (LANES - start) % LANES, 1) if start else part
                ends[1, b, rows, :] = own[b, rows, 0:LANES] + jnp.where(lane < 16, part, 0.0)
                part = fixes[0][8 * b : 8 * (b + 1), tile]
                part = pltpu.roll(part, 112 - start, 1) if start < 112 else part
                ends[0, b, rows, :] = own[b, rows, 2 * LANES : OUT] + jnp.where(lane >= 112, part, 0.0)
        for end in (0, 1):
            bs = pl.ds(2 * p, 2)
            lanes = pl.ds(0 if end else 2 * LANES, LANES)
            copies.append(pltpu.make_async_copy(ends.at[end, bs], out.at[bs, :, lanes], sems.at[len(copies)]))
            copies[-1].start()
    for copy in copies:
        copy.wait()


def scoped(n_xl, n_ta, *refs):
    pl.run_scoped(
        lambda load_sem, send_sem: kernel(load_sem, send_sem, n_xl, n_ta, *refs),
        pltpu.SemaphoreType.DMA((5 + len(BLOCKS),)),
        pltpu.SemaphoreType.DMA((len(OFFSETS),)),
    )


def solution(mesh):
    n_xl, n_ta = mesh.shape["xl"], mesh.shape["ta"]
    tables = filter_table(), halo_table()
    f32 = jnp.float32

    def shards(traces, steps):
        found = pl.pallas_call(
            functools.partial(scoped, n_xl, n_ta),
            name="stack_resample",
            out_shape=(
                jax.ShapeDtypeStruct((BROWS, BCOLS, OUT), f32),
                jax.ShapeDtypeStruct((2, 2, SPAN, SPAN), jnp.bfloat16),
                jax.ShapeDtypeStruct((2, BROWS, 8, LANES), f32),
                jax.ShapeDtypeStruct((2, BROWS, 8, LANES), f32),
                jax.ShapeDtypeStruct((2, 8, LANES), f32),
                jax.ShapeDtypeStruct((2, 2, BROWS, LANES), f32),
                jax.ShapeDtypeStruct((2, 2, 1, LANES), f32),
            ),
            in_specs=[pl.BlockSpec(memory_space=pltpu.HBM)] * 4,
            out_specs=(pl.BlockSpec(memory_space=pltpu.VMEM),) * 7,
            scratch_shapes=[
                pltpu.VMEM((ROWS, COLS, SPAN), f32),
                pltpu.VMEM((2, ROWS, 8, SPAN), f32),
                pltpu.VMEM((2, ROWS, COLS), jnp.int32),
                pltpu.VMEM((2, ROWS, SPAN), jnp.int32),
                pltpu.VMEM((3, SPAN, SPAN), jnp.bfloat16),
                pltpu.VMEM((BROWS, 3 * HALVES[0], SPAN), jnp.bfloat16),
                pltpu.VMEM((BROWS, 3 * HALVES[1], SPAN), jnp.bfloat16),
                pltpu.VMEM((BROWS + 2, HELD, OUT), f32),
                pltpu.VMEM((2, 2 * BROWS, OUT), f32),
                pltpu.VMEM((2, BROWS, 8, LANES), f32),
                pltpu.VMEM((2, 8, LANES), f32),
                pltpu.VMEM((HELD, OUT), f32),
                pltpu.VMEM((2, BROWS, OUT), f32),
                pltpu.VMEM((2, 1, OUT), f32),
                pltpu.SemaphoreType.DMA((len(OFFSETS),)),
            ],
            compiler_params=pltpu.CompilerParams(
                collective_id=0, has_side_effects=True, vmem_limit_bytes=32 * 1024 * 1024
            ),
        )(*(pltpu.with_memory_space_constraint(a, pltpu.HBM) for a in (traces, steps, *map(jnp.asarray, tables))))
        return pl.pallas_call(
            lambda *refs: pl.run_scoped(
                lambda sems: finish(sems, *refs), pltpu.SemaphoreType.DMA((1 + BROWS,))
            ),
            name="finish",
            out_shape=jax.ShapeDtypeStruct((BROWS, BCOLS, OUT), f32),
            in_specs=[pl.BlockSpec(memory_space=pltpu.VMEM)] * 7,
            out_specs=pl.BlockSpec(memory_space=pltpu.HBM),
            scratch_shapes=[
                pltpu.VMEM((2, BROWS, BCOLS, LANES), f32),
            ],
            compiler_params=pltpu.CompilerParams(vmem_limit_bytes=16 * 1024 * 1024),
        )(*found)

    return jax.shard_map(
        shards,
        mesh=mesh,
        in_specs=(P("il", "xl", "ta"), P(None, "il", "xl")),
        out_specs=P("il", "xl", "ta"),
        check_vma=False,
    )
```

```python
import functools

import jax
import jax.numpy as jnp
import numpy as np
from jax import lax
from jax.experimental import pallas as pl
from jax.experimental.pallas import tpu as pltpu
from jax.sharding import PartitionSpec as P

TAPS = 16
P_SIZE = 3
Q = 2
REACH = TAPS // 2

LANES = 128
ROWS, COLS, SPAN = 16, 208, 256
BROWS, BCOLS, OUT = 8, 104, 384
HALVES = (64, 48)
STARTS = (0, 64)
HELD = 112
SPLIT = 56
FIRST_BIN, LAST_BIN = 0, 111
WINDOWS = ((0, 120), (104, 208))
GROUPS = tuple(range(0, 56, 8)) + tuple(range(64, 112, 8))

OFFSETS = tuple(
    (di, dx, dt) for di in (0, 1) for dx in (-1, 0, 1) for dt in (-1, 0, 1) if (di, dx, dt) != (0, 0, 0)
)


SIDES = ((-1, -1), (-1, 1), (1, -1), (1, 1), (0, -1), (0, 1), (-1, 0), (1, 0), (0, 0))
EARLY = SIDES[:4] + SIDES[6:8]
LATE = SIDES[4:6] + SIDES[8:]
BLOCKS = (range(0, 3), range(3, 8))


def filter_table():
    lane = np.arange(LANES)
    sample = np.stack(
        [
            np.where(lane < 112, lane, lane - 128),
            np.where(lane < 64, lane + 128, lane),
            np.where(lane < 16, lane + 256, lane + 128),
        ]
    )
    output = np.arange(OUT).reshape(3, LANES)
    x = (Q * output[:, None, :] - P_SIZE * sample[:, :, None]) / P_SIZE
    weights = np.where(np.abs(x) < REACH, np.sinc(x) * np.sinc(x / REACH), 0.0).astype(np.float32)
    high = weights.astype(jnp.bfloat16)
    low = (weights - high.astype(np.float32)).astype(jnp.bfloat16)
    top = np.concatenate([high, low], axis=2)
    bottom = np.concatenate([high, np.zeros_like(low)], axis=2)
    return np.concatenate([top, bottom], axis=1)


def halo_table():
    sample = np.arange(8)[:, None]
    weights = np.zeros((2, LANES, SPAN), np.float32)
    for end in (0, 1):
        n = sample - 8 if end else sample + SPAN
        x = (Q * (np.arange(16)[None, :] + (0 if end else OUT - 16)) - P_SIZE * n) / P_SIZE
        part = np.where(np.abs(x) < REACH, np.sinc(x) * np.sinc(x / REACH), 0.0)
        for r in range(len(GROUPS)):
            first = (8 * r + 120 * end) % LANES
            weights[end, first : first + 8, 16 * r : 16 * (r + 1)] = part
    high = weights.astype(jnp.bfloat16)
    low = (weights - high.astype(np.float32)).astype(jnp.bfloat16)
    return np.stack(
        [np.concatenate([high, high], axis=1), np.concatenate([low, np.zeros_like(low)], axis=1)], axis=1
    )


def in_group(r, end):
    start = (8 * r + (120 if end else 0)) % LANES
    lane = lax.broadcasted_iota(jnp.int32, (8, LANES), 1)
    return (lane >= start) & (lane < start + 8)


def parts_of(values):
    high = values.astype(jnp.bfloat16)
    low = (values - high.astype(jnp.float32)).astype(jnp.bfloat16)
    return high, low


def both(*conditions):
    held = [c for c in conditions if c is not None]
    return functools.reduce(jnp.logical_and, held) if held else None


def kernel(
    load_sem, send_sem, n_xl, n_ta, traces, steps, table, ends_table, out, tab_ends, scale_packed, fixes, rf, rg,
    x, edges, sv, cbuf, tab, onehot0, onehot1, acc, rims, packed, packed_rim,
    ra, rb, rc, rd, re, recv_sem,
):
    il, xl, ta = lax.axis_index("il"), lax.axis_index("xl"), lax.axis_index("ta")

    def there(step, index, size):
        return None if step == 0 else (index > 0 if step < 0 else index < size - 1)

    def device(offset):
        return {"il": 1 - il if offset[0] else il, "xl": xl + offset[1], "ta": ta + offset[2]}

    def for_neighbours(sides, action, sign=1):
        for dx, dt in sides:
            condition = both(there(sign * dx, xl, n_xl), there(sign * dt, ta, n_ta))

            def run(dx=dx, dt=dt):
                for di in (0, 1):
                    if (di, dx, dt) != (0, 0, 0):
                        action((di, dx, dt))

            if condition is None:
                run()
            else:
                pl.when(condition)(run)

    barrier = pltpu.get_barrier_semaphore()

    def greet(offset):
        pl.semaphore_signal(
            barrier, 1, device_id=device(offset), device_id_type=pl.DeviceIdType.MESH
        )

    for_neighbours(SIDES, greet)

    steps_copy = pltpu.make_async_copy(steps, sv, load_sem.at[0])
    steps_copy.start()
    edge_copies = []
    for side in (0, 1):
        columns = pl.ds((COLS - 8) * side, 8)
        edge_copies.append(pltpu.make_async_copy(traces.at[:, columns, :], edges.at[side], load_sem.at[1 + side]))
        edge_copies[-1].start()
    loads = []
    for block in BLOCKS:
        rows = pl.ds(2 * block[0], 2 * len(block))
        loads.append(pltpu.make_async_copy(traces.at[rows], x.at[rows], load_sem.at[3 + len(loads)]))
        loads[-1].start()
    table_copies = [
        pltpu.make_async_copy(table, tab, load_sem.at[3 + len(BLOCKS)]),
        pltpu.make_async_copy(ends_table, tab_ends, load_sem.at[4 + len(BLOCKS)]),
    ]
    for copy in table_copies:
        copy.start()

    edge = (1 - il) * (BROWS + 1)
    target = BROWS - (BROWS - 1) * il

    own, far = pl.ds(0, BROWS), pl.ds(BROWS, 1)
    copies = {}
    for number, offset in enumerate(OFFSETS):
        di, dx, dt = offset
        side, end = (dx + 1) // 2, (dt + 1) // 2
        lanes = pl.ds(LANES * end, LANES)
        if dt == 0 and dx == 0:
            source, place = acc.at[edge], ra
        elif dt == 0:
            source, place = (rims.at[side, far], rc.at[side]) if di else (rims.at[side, own], rb.at[side])
        elif dx == 0:
            source, place = (packed_rim.at[end], re.at[end]) if di else (packed.at[end], rd.at[end])
        elif di:
            source, place = rims.at[side, far, lanes], rg.at[end, side]
        else:
            source, place = rims.at[side, own, lanes], rf.at[end, side]
        copies[offset] = pltpu.make_async_remote_copy(
            src_ref=source,
            dst_ref=place,
            send_sem=send_sem.at[number],
            recv_sem=recv_sem.at[number],
            device_id=device(offset),
            device_id_type=pl.DeviceIdType.MESH,
        )

    for dx in (-1, 1):
        side = (dx + 1) // 2

        @pl.when(jnp.logical_not(there(-dx, xl, n_xl)))
        def _(side=side):
            for place in (rb.at[side], rc.at[side], *(r.at[e, side] for r in (rf, rg) for e in (0, 1))):
                place[...] = jnp.zeros(place.shape, jnp.float32)

    for dt in (-1, 1):
        end = (dt + 1) // 2

        @pl.when(jnp.logical_not(there(-dt, ta, n_ta)))
        def _(end=end):
            for place in (rd.at[end], re.at[end], rf.at[end], rg.at[end]):
                place[...] = jnp.zeros(place.shape, jnp.float32)

    steps_copy.wait()
    row_bin = lax.shift_right_logical(lax.broadcasted_iota(jnp.int32, (ROWS, COLS), 0), 1) + sv[0]
    inside = (row_bin >= 0) & (row_bin < BROWS)
    row_code = jnp.where(inside, row_bin, jnp.where(row_bin == edge - 1, BROWS, -1))
    wide = lax.broadcasted_iota(jnp.int32, (ROWS, SPAN), 1)
    bin_col = lax.shift_right_logical(lax.broadcasted_iota(jnp.int32, (ROWS, COLS), 1), 1) + sv[1]
    cbuf[...] = jnp.full(cbuf.shape, -1, jnp.int32)
    cbuf[0, :, 0:COLS] = jnp.where(
        (bin_col >= 0) & (bin_col < SPLIT), (sv[0] + 1) * HALVES[0] + bin_col, -1
    )
    cbuf[1, :, 0:COLS] = jnp.where(
        (bin_col >= SPLIT) & (bin_col < BCOLS), (sv[0] + 1) * HALVES[1] + bin_col - SPLIT, -1
    )
    first, second = cbuf[0], cbuf[1]
    codes = (
        (
            jnp.where(wide < 120, first, -1),
            jnp.where((wide >= 120) & (wide < 240), pltpu.roll(first, 120, 1), -1),
        ),
        (
            jnp.where(wide < 104, pltpu.roll(second, SPAN - 104, 1), -1),
            jnp.where((wide >= 104) & (wide < 208), second, -1),
        ),
    )
    onehot = (onehot0, onehot1)
    for h, size in enumerate(HALVES):
        places = lax.broadcasted_iota(jnp.int32, (3 * size, SPAN), 0)
        even, odd = codes[h]
        for k in range(BROWS):
            code = jnp.maximum(even[2 * k : 2 * k + 1], odd[2 * k + 1 : 2 * k + 2])
            onehot[h][k] = jnp.where(places == code, 1.0, 0.0).astype(jnp.bfloat16)

    for b in range(BROWS + 2):
        for h, size in enumerate(HALVES):
            rows = [onehot[h][k, size * (b - k) : size * (b - k + 1), :] for k in range(BROWS) if 0 <= b - k < 3]
            total = functools.reduce(jnp.add, rows)
            total = (total[:, :LANES] + total[:, LANES:]).astype(jnp.float32)
            acc[b, STARTS[h] : STARTS[h] + size, SPAN:OUT] = jnp.broadcast_to(
                jnp.sum(total, axis=1, keepdims=True), (size, LANES)
            )

    lane = lax.broadcasted_iota(jnp.int32, (8, LANES), 1)
    def pack(b, end):
        tile = pl.ds(LANES * end, LANES)
        total = acc[b, 0:8, tile]
        for r in range(1, len(GROUPS)):
            turned = pltpu.roll(acc[b, GROUPS[r] : GROUPS[r] + 8, tile], 8 * r, 1)
            total = jnp.where(in_group(r, end), turned, total)
        return total

    def send(offset):
        copies[offset].start()

    def find_rims():
        slots = lax.broadcasted_iota(jnp.int32, (ROWS, 2 * BROWS), 1)
        ones = jnp.ones((2 * ROWS, LANES), jnp.float32)
        for side in (0, 1):
            code = jnp.where(sv[1] == 2 * side - 1, row_code, -1)
            chosen, values = [], []
            for j in (0, 1):
                column = (COLS - 2) * side + j
                chosen.append(jnp.where(slots == code[:, column : column + 1], 1.0, 0.0))
                values.append(edges[side, :, 6 * side + j, :])
            rims[side] = lax.dot_general(
                jnp.concatenate(chosen, axis=0),
                jnp.concatenate([jnp.concatenate(values, axis=0), ones], axis=1),
                (((0,), (0,)), ((), ())),
                precision=lax.Precision.HIGHEST,
                preferred_element_type=jnp.float32,
            )

    distant = (lax.rem(ta, 4) == 0) | (ta == n_ta // 2 - 1)

    def meet():
        beside_xl = 1 + (xl > 0).astype(jnp.int32) + (xl < n_xl - 1).astype(jnp.int32)
        beside_ta = 1 + (ta > 0).astype(jnp.int32) + (ta < n_ta - 1).astype(jnp.int32)
        pl.semaphore_wait(barrier, 2 * beside_xl * beside_ta - 1)

    for block, load in zip(BLOCKS, loads):
        load.wait()
        if block is BLOCKS[0]:
            for copy in edge_copies:
                copy.wait()
            find_rims()
        for k in block:
            for h, size in enumerate(HALVES):
                start, stop = WINDOWS[h]
                pieces = [x[2 * k, start:stop, :], x[2 * k + 1, start:stop, :]]
                pieces.append(jnp.zeros((SPAN - 2 * (stop - start), SPAN), jnp.float32))
                high, low = parts_of(jnp.concatenate(pieces, axis=0))
                chosen = onehot[h][k]
                result = jnp.dot(chosen, high, preferred_element_type=jnp.float32)
                result = result + jnp.dot(chosen, low, preferred_element_type=jnp.float32)
                for q in range(3):
                    b = k + q
                    where = (b, pl.ds(STARTS[h], size), pl.ds(0, SPAN))
                    part = result[size * q : size * (q + 1)]
                    acc[where] = part if k == max(b - 2, 0) else acc[where] + part
            if k > 0:
                for end in (0, 1):
                    packed[end, k - 1] = pack(k, end)
        if block is BLOCKS[0]:

            @pl.when(jnp.logical_not(distant))
            def _():
                meet()
                for_neighbours(EARLY, send)

    for end in (0, 1):
        packed[end, BROWS - 1] = pack(BROWS, end)
        packed_rim[end] = pack(edge, end)

    @pl.when(distant)
    def _():
        meet()
        for_neighbours(EARLY, send)

    for_neighbours(LATE, send)

    for_neighbours(SIDES[6:], lambda offset: copies[offset].wait_recv(), -1)
    acc[target] = acc[target] + ra[...]
    for row, side in ((FIRST_BIN, 1), (LAST_BIN, 0)):
        acc[target, row : row + 1, :] = acc[target, row : row + 1, :] + rc[side]
        for b in range(BROWS):
            acc[b + 1, row : row + 1, :] = acc[b + 1, row : row + 1, :] + rb[side, b : b + 1, :]

    for copy in table_copies:
        copy.wait()

    def bins(b, tile):
        lanes = pl.ds(LANES * tile, LANES)
        return [acc[b, 0:SPLIT, lanes], acc[b, STARTS[1] : HELD, lanes]]

    def pair(p, tile):
        return jnp.concatenate(bins(2 * p + 1, tile) + bins(2 * p + 2, tile), axis=0)

    across = lax.broadcasted_iota(jnp.int32, (2 * BCOLS, LANES), 1)

    def resample(p, third, window):
        high, low = parts_of(window)
        result = jnp.dot(
            jnp.concatenate([high, low], axis=1), tab[third], preferred_element_type=jnp.float32
        )
        result = result[:, :LANES] + result[:, LANES:]
        lanes = pl.ds(LANES * third, LANES)
        out[2 * p, :, lanes] = result[:BCOLS]
        out[2 * p + 1, :, lanes] = result[BCOLS:]

    for p in range(BROWS // 2):
        factor = 1.0 / jnp.maximum(pair(p, 2), 1.0)
        low, high = pair(p, 0), pair(p, 1)
        resample(p, 1, jnp.where(across < 64, high, low) * factor)
        resample(p, 0, jnp.where(across < 112, low, 0.0) * factor)
        resample(p, 2, jnp.where(across < 16, 0.0, high) * factor)
        for b in (0, 1):
            for end in (0, 1):
                total = jnp.zeros((8, LANES), jnp.float32)
                for r in range(len(GROUPS)):
                    row = BCOLS * b + 8 * r
                    total = jnp.where(in_group(r, end), factor[row : row + 8], total)
                scale_packed[end, 2 * p + b] = total
    for_neighbours(SIDES, lambda offset: copies[offset].wait_send())

    for_neighbours(SIDES[4:6], lambda offset: copies[offset].wait_recv(), -1)
    for end in (0, 1):
        rows = []
        for b in range(BROWS):
            tile = rd[end, b]
            if b in (0, BROWS - 1):
                tile = tile + jnp.where(target == b + 1, re[end], 0.0)
            rows.append(tile * scale_packed[end, b])
        fixes[end] = halo_product(jnp.concatenate(rows, axis=0), tab_ends, end)
    for_neighbours(SIDES[:4], lambda offset: copies[offset].wait_recv(), -1)


def halo_product(packed, tab_ends, end):
    high, low = parts_of(packed)
    halves = jnp.concatenate([high, low], axis=1)
    result = jnp.dot(halves, tab_ends[end, 0], preferred_element_type=jnp.float32)
    return result + jnp.dot(halves, tab_ends[end, 1], preferred_element_type=jnp.float32)


def finish(sems, own, tab_ends, scale_packed, fixes, rf, rg, out, ends):
    middle = pl.ds(LANES, LANES)
    copies = [pltpu.make_async_copy(own.at[:, :, middle], out.at[:, :, middle], sems.at[0])]
    copies[0].start()
    lane = lax.broadcasted_iota(jnp.int32, (8, LANES), 1)
    sublane = lax.broadcasted_iota(jnp.int32, (8, LANES), 0)
    target = BROWS - (BROWS - 1) * lax.axis_index("il")

    last = len(GROUPS) - 1

    def rims(end):
        rows = []
        for r, side, line in ((0, 1, 0), (last, 0, 7)):
            near, far = rf[end, side], jnp.broadcast_to(rg[end, side], (8, LANES))
            both = near + jnp.where(sublane == target - 1, far, 0.0)
            both = pltpu.roll(both, 8 * r, 1) if r else both
            rows.append(jnp.where(in_group(r, end), both, 0.0) * scale_packed[end, :, line, :])
        result = halo_product(jnp.concatenate(rows, axis=0), tab_ends, end)
        return result[:8, :LANES], result[8:, LANES:]

    added = rims(0), rims(1)

    def part_of(b, r, end):
        tile = slice(LANES * (r // 8), LANES * (r // 8 + 1))
        part = fixes[end, 8 * b : 8 * (b + 1), tile]
        if r in (0, last):
            here = sublane == (0 if r == 0 else 7)
            part = part + jnp.where(here, added[end][0 if r == 0 else 1][b : b + 1], 0.0)
        turn = ((0 if end else 112) - 16 * (r % 8)) % LANES
        part = pltpu.roll(part, turn, 1) if turn else part
        return jnp.where(lane < 16 if end else lane >= 112, part, 0.0)

    for p in range(BROWS // 2):
        for b in (2 * p, 2 * p + 1):
            for r in range(len(GROUPS)):
                rows = pl.ds(8 * r, 8)
                ends[1, b, rows, :] = own[b, rows, 0:LANES] + part_of(b, r, 1)
                ends[0, b, rows, :] = own[b, rows, 2 * LANES : OUT] + part_of(b, r, 0)
        for end in (0, 1):
            bs = pl.ds(2 * p, 2)
            lanes = pl.ds(0 if end else 2 * LANES, LANES)
            copies.append(pltpu.make_async_copy(ends.at[end, bs], out.at[bs, :, lanes], sems.at[len(copies)]))
            copies[-1].start()
    for copy in copies:
        copy.wait()


def scoped(n_xl, n_ta, *refs):
    pl.run_scoped(
        lambda load_sem, send_sem: kernel(load_sem, send_sem, n_xl, n_ta, *refs),
        pltpu.SemaphoreType.DMA((5 + len(BLOCKS),)),
        pltpu.SemaphoreType.DMA((len(OFFSETS),)),
    )


def solution(mesh):
    n_xl, n_ta = mesh.shape["xl"], mesh.shape["ta"]
    tables = filter_table(), halo_table()
    f32 = jnp.float32

    def shards(traces, steps):
        found = pl.pallas_call(
            functools.partial(scoped, n_xl, n_ta),
            name="stack_resample",
            out_shape=(
                jax.ShapeDtypeStruct((BROWS, BCOLS, OUT), f32),
                jax.ShapeDtypeStruct((2, 2, SPAN, SPAN), jnp.bfloat16),
                jax.ShapeDtypeStruct((2, BROWS, 8, LANES), f32),
                jax.ShapeDtypeStruct((2, 8 * BROWS, SPAN), f32),
                jax.ShapeDtypeStruct((2, 2, BROWS, LANES), f32),
                jax.ShapeDtypeStruct((2, 2, 1, LANES), f32),
            ),
            in_specs=[pl.BlockSpec(memory_space=pltpu.HBM)] * 4,
            out_specs=(pl.BlockSpec(memory_space=pltpu.VMEM),) * 6,
            scratch_shapes=[
                pltpu.VMEM((ROWS, COLS, SPAN), f32),
                pltpu.VMEM((2, ROWS, 8, SPAN), f32),
                pltpu.VMEM((2, ROWS, COLS), jnp.int32),
                pltpu.VMEM((2, ROWS, SPAN), jnp.int32),
                pltpu.VMEM((3, SPAN, SPAN), jnp.bfloat16),
                pltpu.VMEM((BROWS, 3 * HALVES[0], SPAN), jnp.bfloat16),
                pltpu.VMEM((BROWS, 3 * HALVES[1], SPAN), jnp.bfloat16),
                pltpu.VMEM((BROWS + 2, HELD, OUT), f32),
                pltpu.VMEM((2, 2 * BROWS, OUT), f32),
                pltpu.VMEM((2, BROWS, 8, LANES), f32),
                pltpu.VMEM((2, 8, LANES), f32),
                pltpu.VMEM((HELD, OUT), f32),
                pltpu.VMEM((2, BROWS, OUT), f32),
                pltpu.VMEM((2, 1, OUT), f32),
                pltpu.VMEM((2, BROWS, 8, LANES), f32),
                pltpu.VMEM((2, 8, LANES), f32),
                pltpu.SemaphoreType.DMA((len(OFFSETS),)),
            ],
            compiler_params=pltpu.CompilerParams(
                collective_id=0, has_side_effects=True, vmem_limit_bytes=32 * 1024 * 1024
            ),
        )(*(pltpu.with_memory_space_constraint(a, pltpu.HBM) for a in (traces, steps, *map(jnp.asarray, tables))))
        return pl.pallas_call(
            lambda *refs: pl.run_scoped(
                lambda sems: finish(sems, *refs), pltpu.SemaphoreType.DMA((1 + BROWS,))
            ),
            name="finish",
            out_shape=jax.ShapeDtypeStruct((BROWS, BCOLS, OUT), f32),
            in_specs=[pl.BlockSpec(memory_space=pltpu.VMEM)] * 6,
            out_specs=pl.BlockSpec(memory_space=pltpu.HBM),
            scratch_shapes=[
                pltpu.VMEM((2, BROWS, BCOLS, LANES), f32),
            ],
            compiler_params=pltpu.CompilerParams(vmem_limit_bytes=16 * 1024 * 1024),
        )(*found)

    return jax.shard_map(
        shards,
        mesh=mesh,
        in_specs=(P("il", "xl", "ta"), P(None, "il", "xl")),
        out_specs=P("il", "xl", "ta"),
        check_vma=False,
    )
```

```python
import functools

import jax
import jax.numpy as jnp
import numpy as np
from jax import lax
from jax.experimental import pallas as pl
from jax.experimental.pallas import tpu as pltpu
from jax.sharding import PartitionSpec as P

TAPS = 16
P_SIZE = 3
Q = 2
REACH = TAPS // 2

LANES = 128
ROWS, COLS, SPAN = 16, 208, 256
BROWS, BCOLS, OUT = 8, 104, 384
HALVES = (64, 48)
STARTS = (0, 64)
HELD = 112
SPLIT = 56
FIRST_BIN, LAST_BIN = 0, 111
WINDOWS = ((0, 120), (104, 208))
GROUPS = tuple(range(0, 56, 8)) + tuple(range(64, 112, 8))

OFFSETS = tuple(
    (di, dx, dt) for di in (0, 1) for dx in (-1, 0, 1) for dt in (-1, 0, 1) if (di, dx, dt) != (0, 0, 0)
)


SIDES = ((-1, -1), (-1, 1), (1, -1), (1, 1), (0, -1), (0, 1), (-1, 0), (1, 0), (0, 0))
EARLY = SIDES[:4] + SIDES[6:8]
LATE = SIDES[4:6] + SIDES[8:]
BLOCKS = (range(0, 3), range(3, 8))


def filter_table():
    lane = np.arange(LANES)
    sample = np.stack(
        [
            np.where(lane < 112, lane, lane - 128),
            np.where(lane < 64, lane + 128, lane),
            np.where(lane < 16, lane + 256, lane + 128),
        ]
    )
    output = np.arange(OUT).reshape(3, LANES)
    x = (Q * output[:, None, :] - P_SIZE * sample[:, :, None]) / P_SIZE
    weights = np.where(np.abs(x) < REACH, np.sinc(x) * np.sinc(x / REACH), 0.0).astype(np.float32)
    high = weights.astype(jnp.bfloat16)
    low = (weights - high.astype(np.float32)).astype(jnp.bfloat16)
    top = np.concatenate([high, low], axis=2)
    bottom = np.concatenate([high, np.zeros_like(low)], axis=2)
    return np.concatenate([top, bottom], axis=1)


def halo_table():
    sample = np.arange(8)[:, None]
    weights = np.zeros((2, LANES, SPAN), np.float32)
    for end in (0, 1):
        n = sample - 8 if end else sample + SPAN
        x = (Q * (np.arange(16)[None, :] + (0 if end else OUT - 16)) - P_SIZE * n) / P_SIZE
        part = np.where(np.abs(x) < REACH, np.sinc(x) * np.sinc(x / REACH), 0.0)
        for r in range(len(GROUPS)):
            first = (8 * r + 120 * end) % LANES
            weights[end, first : first + 8, 16 * r : 16 * (r + 1)] = part
    high = weights.astype(jnp.bfloat16)
    low = (weights - high.astype(np.float32)).astype(jnp.bfloat16)
    return np.stack(
        [np.concatenate([high, high], axis=1), np.concatenate([low, np.zeros_like(low)], axis=1)], axis=1
    )


def rim_table():
    weights = np.zeros((2, LANES, LANES), np.float32)
    sample = np.arange(8)[:, None]
    for end in (0, 1):
        n = sample - 8 if end else sample + SPAN
        x = (Q * (np.arange(16)[None, :] + (0 if end else OUT - 16)) - P_SIZE * n) / P_SIZE
        part = np.where(np.abs(x) < REACH, np.sinc(x) * np.sinc(x / REACH), 0.0)
        first, place = (LANES - 8, 0) if end else (0, LANES - 16)
        weights[end, first : first + 8, place : place + 16] = part
    return weights


def in_group(r, end):
    start = (8 * r + (120 if end else 0)) % LANES
    lane = lax.broadcasted_iota(jnp.int32, (8, LANES), 1)
    return (lane >= start) & (lane < start + 8)


def parts_of(values):
    high = values.astype(jnp.bfloat16)
    low = (values - high.astype(jnp.float32)).astype(jnp.bfloat16)
    return high, low


def both(*conditions):
    held = [c for c in conditions if c is not None]
    return functools.reduce(jnp.logical_and, held) if held else None


def kernel(
    load_sem, send_sem, n_xl, n_ta, traces, steps, table, ends_table, rims_table, out, rim_scale, fixes, rf, rg,
    x, edges, sv, cbuf, tab, tab_ends, tab_rims, onehot0, onehot1, acc, scale_packed, rims, reach, packed, packed_rim,
    ra, rb, rc, rd, re, recv_sem,
):
    il, xl, ta = lax.axis_index("il"), lax.axis_index("xl"), lax.axis_index("ta")

    def there(step, index, size):
        return None if step == 0 else (index > 0 if step < 0 else index < size - 1)

    def device(offset):
        return {"il": 1 - il if offset[0] else il, "xl": xl + offset[1], "ta": ta + offset[2]}

    def for_neighbours(sides, action, sign=1):
        for dx, dt in sides:
            condition = both(there(sign * dx, xl, n_xl), there(sign * dt, ta, n_ta))

            def run(dx=dx, dt=dt):
                for di in (0, 1):
                    if (di, dx, dt) != (0, 0, 0):
                        action((di, dx, dt))

            if condition is None:
                run()
            else:
                pl.when(condition)(run)

    barrier = pltpu.get_barrier_semaphore()

    def greet(offset):
        pl.semaphore_signal(
            barrier, 1, device_id=device(offset), device_id_type=pl.DeviceIdType.MESH
        )

    for_neighbours(SIDES, greet)

    steps_copy = pltpu.make_async_copy(steps, sv, load_sem.at[0])
    steps_copy.start()
    edge_copies = []
    for side in (0, 1):
        columns = pl.ds((COLS - 8) * side, 8)
        edge_copies.append(pltpu.make_async_copy(traces.at[:, columns, :], edges.at[side], load_sem.at[1 + side]))
        edge_copies[-1].start()
    edge_copies.append(pltpu.make_async_copy(rims_table, tab_rims, load_sem.at[5 + len(BLOCKS)]))
    edge_copies[-1].start()
    loads = []
    for block in BLOCKS:
        rows = pl.ds(2 * block[0], 2 * len(block))
        loads.append(pltpu.make_async_copy(traces.at[rows], x.at[rows], load_sem.at[3 + len(loads)]))
        loads[-1].start()
    table_copies = [
        pltpu.make_async_copy(table, tab, load_sem.at[3 + len(BLOCKS)]),
        pltpu.make_async_copy(ends_table, tab_ends, load_sem.at[4 + len(BLOCKS)]),
    ]
    for copy in table_copies:
        copy.start()

    edge = (1 - il) * (BROWS + 1)
    target = BROWS - (BROWS - 1) * il

    own, far = pl.ds(0, BROWS), pl.ds(BROWS, 1)
    copies = {}
    for number, offset in enumerate(OFFSETS):
        di, dx, dt = offset
        side, end = (dx + 1) // 2, (dt + 1) // 2
        if dt == 0 and dx == 0:
            source, place = acc.at[edge], ra
        elif dt == 0:
            source, place = (rims.at[side, far], rc.at[side]) if di else (rims.at[side, own], rb.at[side])
        elif dx == 0:
            source, place = (packed_rim.at[end], re.at[end]) if di else (packed.at[end], rd.at[end])
        elif di:
            source, place = reach.at[end, side, far], rg.at[end, side]
        else:
            source, place = reach.at[end, side, own], rf.at[end, side]
        copies[offset] = pltpu.make_async_remote_copy(
            src_ref=source,
            dst_ref=place,
            send_sem=send_sem.at[number],
            recv_sem=recv_sem.at[number],
            device_id=device(offset),
            device_id_type=pl.DeviceIdType.MESH,
        )

    for dx in (-1, 1):
        side = (dx + 1) // 2

        @pl.when(jnp.logical_not(there(-dx, xl, n_xl)))
        def _(side=side):
            for place in (rb.at[side], rc.at[side], *(r.at[e, side] for r in (rf, rg) for e in (0, 1))):
                place[...] = jnp.zeros(place.shape, jnp.float32)

    for dt in (-1, 1):
        end = (dt + 1) // 2

        @pl.when(jnp.logical_not(there(-dt, ta, n_ta)))
        def _(end=end):
            for place in (rd.at[end], re.at[end], rf.at[end], rg.at[end]):
                place[...] = jnp.zeros(place.shape, jnp.float32)

    for copy in (steps_copy, *edge_copies):
        copy.wait()
    row_bin = lax.shift_right_logical(lax.broadcasted_iota(jnp.int32, (ROWS, COLS), 0), 1) + sv[0]
    inside = (row_bin >= 0) & (row_bin < BROWS)
    row_code = jnp.where(inside, row_bin, jnp.where(row_bin == edge - 1, BROWS, -1))
    def find_rims():
        slots = lax.broadcasted_iota(jnp.int32, (ROWS, 2 * BROWS), 1)
        ones = jnp.ones((2 * ROWS, LANES), jnp.float32)
        for side in (0, 1):
            code = jnp.where(sv[1] == 2 * side - 1, row_code, -1)
            chosen, values = [], []
            for j in (0, 1):
                column = (COLS - 2) * side + j
                chosen.append(jnp.where(slots == code[:, column : column + 1], 1.0, 0.0))
                values.append(edges[side, :, 6 * side + j, :])
            rims[side] = lax.dot_general(
                jnp.concatenate(chosen, axis=0),
                jnp.concatenate([jnp.concatenate(values, axis=0), ones], axis=1),
                (((0,), (0,)), ((), ())),
                precision=lax.Precision.HIGHEST,
                preferred_element_type=jnp.float32,
            )
        for end in (0, 1):
            tiles = [rims[side, :, LANES * end : LANES * (end + 1)] for side in (0, 1)]
            product = jnp.dot(
                jnp.concatenate(tiles, axis=0),
                tab_rims[end],
                precision=lax.Precision.HIGHEST,
                preferred_element_type=jnp.float32,
            )
            for side in (0, 1):
                reach[end, side] = product[2 * BROWS * side : 2 * BROWS * (side + 1)]

    find_rims()

    wide = lax.broadcasted_iota(jnp.int32, (ROWS, SPAN), 1)
    bin_col = lax.shift_right_logical(lax.broadcasted_iota(jnp.int32, (ROWS, COLS), 1), 1) + sv[1]
    cbuf[...] = jnp.full(cbuf.shape, -1, jnp.int32)
    cbuf[0, :, 0:COLS] = jnp.where(
        (bin_col >= 0) & (bin_col < SPLIT), (sv[0] + 1) * HALVES[0] + bin_col, -1
    )
    cbuf[1, :, 0:COLS] = jnp.where(
        (bin_col >= SPLIT) & (bin_col < BCOLS), (sv[0] + 1) * HALVES[1] + bin_col - SPLIT, -1
    )
    first, second = cbuf[0], cbuf[1]
    codes = (
        (
            jnp.where(wide < 120, first, -1),
            jnp.where((wide >= 120) & (wide < 240), pltpu.roll(first, 120, 1), -1),
        ),
        (
            jnp.where(wide < 104, pltpu.roll(second, SPAN - 104, 1), -1),
            jnp.where((wide >= 104) & (wide < 208), second, -1),
        ),
    )
    onehot = (onehot0, onehot1)
    for h, size in enumerate(HALVES):
        places = lax.broadcasted_iota(jnp.int32, (3 * size, SPAN), 0)
        even, odd = codes[h]
        for k in range(BROWS):
            code = jnp.maximum(even[2 * k : 2 * k + 1], odd[2 * k + 1 : 2 * k + 2])
            onehot[h][k] = jnp.where(places == code, 1.0, 0.0).astype(jnp.bfloat16)

    for b in range(BROWS + 2):
        for h, size in enumerate(HALVES):
            rows = [onehot[h][k, size * (b - k) : size * (b - k + 1), :] for k in range(BROWS) if 0 <= b - k < 3]
            total = functools.reduce(jnp.add, rows)
            total = (total[:, :LANES] + total[:, LANES:]).astype(jnp.float32)
            acc[b, STARTS[h] : STARTS[h] + size, SPAN:OUT] = jnp.broadcast_to(
                jnp.sum(total, axis=1, keepdims=True), (size, LANES)
            )

    lane = lax.broadcasted_iota(jnp.int32, (8, LANES), 1)
    def pack(b, end):
        tile = pl.ds(LANES * end, LANES)
        total = acc[b, 0:8, tile]
        for r in range(1, len(GROUPS)):
            turned = pltpu.roll(acc[b, GROUPS[r] : GROUPS[r] + 8, tile], 8 * r, 1)
            total = jnp.where(in_group(r, end), turned, total)
        return total

    def send(offset):
        copies[offset].start()

    distant = (lax.rem(ta, 4) == 0) | (ta == n_ta // 2 - 1)

    def meet():
        beside_xl = 1 + (xl > 0).astype(jnp.int32) + (xl < n_xl - 1).astype(jnp.int32)
        beside_ta = 1 + (ta > 0).astype(jnp.int32) + (ta < n_ta - 1).astype(jnp.int32)
        pl.semaphore_wait(barrier, 2 * beside_xl * beside_ta - 1)

    for block, load in zip(BLOCKS, loads):
        load.wait()
        for k in block:
            for h, size in enumerate(HALVES):
                start, stop = WINDOWS[h]
                pieces = [x[2 * k, start:stop, :], x[2 * k + 1, start:stop, :]]
                pieces.append(jnp.zeros((SPAN - 2 * (stop - start), SPAN), jnp.float32))
                high, low = parts_of(jnp.concatenate(pieces, axis=0))
                chosen = onehot[h][k]
                result = jnp.dot(chosen, high, preferred_element_type=jnp.float32)
                result = result + jnp.dot(chosen, low, preferred_element_type=jnp.float32)
                for q in range(3):
                    b = k + q
                    where = (b, pl.ds(STARTS[h], size), pl.ds(0, SPAN))
                    part = result[size * q : size * (q + 1)]
                    acc[where] = part if k == max(b - 2, 0) else acc[where] + part
            if k > 0:
                for end in (0, 1):
                    packed[end, k - 1] = pack(k, end)
        if block is BLOCKS[0]:

            @pl.when(jnp.logical_not(distant))
            def _():
                meet()
                for_neighbours(EARLY, send)

    for end in (0, 1):
        packed[end, BROWS - 1] = pack(BROWS, end)
        packed_rim[end] = pack(edge, end)

    @pl.when(distant)
    def _():
        meet()
        for_neighbours(EARLY, send)

    for_neighbours(LATE, send)

    for_neighbours(SIDES[6:], lambda offset: copies[offset].wait_recv(), -1)
    acc[target] = acc[target] + ra[...]
    for row, side in ((FIRST_BIN, 1), (LAST_BIN, 0)):
        acc[target, row : row + 1, :] = acc[target, row : row + 1, :] + rc[side]
        for b in range(BROWS):
            acc[b + 1, row : row + 1, :] = acc[b + 1, row : row + 1, :] + rb[side, b : b + 1, :]

    for copy in table_copies:
        copy.wait()

    def bins(b, tile):
        lanes = pl.ds(LANES * tile, LANES)
        return [acc[b, 0:SPLIT, lanes], acc[b, STARTS[1] : HELD, lanes]]

    def pair(p, tile):
        return jnp.concatenate(bins(2 * p + 1, tile) + bins(2 * p + 2, tile), axis=0)

    across = lax.broadcasted_iota(jnp.int32, (2 * BCOLS, LANES), 1)

    def resample(p, third, window):
        high, low = parts_of(window)
        result = jnp.dot(
            jnp.concatenate([high, low], axis=1), tab[third], preferred_element_type=jnp.float32
        )
        result = result[:, :LANES] + result[:, LANES:]
        lanes = pl.ds(LANES * third, LANES)
        out[2 * p, :, lanes] = result[:BCOLS]
        out[2 * p + 1, :, lanes] = result[BCOLS:]

    for p in range(BROWS // 2):
        factor = 1.0 / jnp.maximum(pair(p, 2), 1.0)
        low, high = pair(p, 0), pair(p, 1)
        resample(p, 1, jnp.where(across < 64, high, low) * factor)
        resample(p, 0, jnp.where(across < 112, low, 0.0) * factor)
        resample(p, 2, jnp.where(across < 16, 0.0, high) * factor)
        for b in (0, 1):
            for n, c in enumerate((0, BCOLS - 1)):
                row = BCOLS * b + c
                rim_scale[n, 2 * p + b : 2 * p + b + 1, :] = factor[row : row + 1]
            for end in (0, 1):
                total = jnp.zeros((8, LANES), jnp.float32)
                for r in range(len(GROUPS)):
                    row = BCOLS * b + 8 * r
                    total = jnp.where(in_group(r, end), factor[row : row + 8], total)
                scale_packed[end, 2 * p + b] = total
    for_neighbours(SIDES, lambda offset: copies[offset].wait_send())

    for_neighbours(SIDES[4:6], lambda offset: copies[offset].wait_recv(), -1)
    for end in (0, 1):
        rows = []
        for b in range(BROWS):
            tile = rd[end, b]
            if b in (0, BROWS - 1):
                tile = tile + jnp.where(target == b + 1, re[end], 0.0)
            rows.append(tile * scale_packed[end, b])
        fixes[end] = halo_product(jnp.concatenate(rows, axis=0), tab_ends, end)
    for_neighbours(SIDES[:4], lambda offset: copies[offset].wait_recv(), -1)


def halo_product(packed, tab_ends, end):
    high, low = parts_of(packed)
    halves = jnp.concatenate([high, low], axis=1)
    result = jnp.dot(halves, tab_ends[end, 0], preferred_element_type=jnp.float32)
    return result + jnp.dot(halves, tab_ends[end, 1], preferred_element_type=jnp.float32)


def finish(sems, own, rim_scale, fixes, rf, rg, out, ends):
    middle = pl.ds(LANES, LANES)
    copies = [pltpu.make_async_copy(own.at[:, :, middle], out.at[:, :, middle], sems.at[0])]
    copies[0].start()
    lane = lax.broadcasted_iota(jnp.int32, (8, LANES), 1)
    sublane = lax.broadcasted_iota(jnp.int32, (8, LANES), 0)
    target = BROWS - (BROWS - 1) * lax.axis_index("il")

    last = len(GROUPS) - 1

    def rims(end, n):
        far = jnp.where(sublane == target - 1, jnp.broadcast_to(rg[end, 1 - n], (8, LANES)), 0.0)
        return (rf[end, 1 - n] + far) * rim_scale[n]

    added = [[rims(end, n) for n in (0, 1)] for end in (0, 1)]

    def part_of(b, r, end):
        tile = slice(LANES * (r // 8), LANES * (r // 8 + 1))
        part = fixes[end, 8 * b : 8 * (b + 1), tile]
        turn = ((0 if end else 112) - 16 * (r % 8)) % LANES
        part = pltpu.roll(part, turn, 1) if turn else part
        part = jnp.where(lane < 16 if end else lane >= 112, part, 0.0)
        if r in (0, last):
            n = min(r, 1)
            part = part + jnp.where(sublane == 7 * n, added[end][n][b : b + 1], 0.0)
        return part

    for p in range(BROWS // 2):
        for b in (2 * p, 2 * p + 1):
            for r in range(len(GROUPS)):
                rows = pl.ds(8 * r, 8)
                ends[1, b, rows, :] = own[b, rows, 0:LANES] + part_of(b, r, 1)
                ends[0, b, rows, :] = own[b, rows, 2 * LANES : OUT] + part_of(b, r, 0)
        for end in (0, 1):
            bs = pl.ds(2 * p, 2)
            lanes = pl.ds(0 if end else 2 * LANES, LANES)
            copies.append(pltpu.make_async_copy(ends.at[end, bs], out.at[bs, :, lanes], sems.at[len(copies)]))
            copies[-1].start()
    for copy in copies:
        copy.wait()


def scoped(n_xl, n_ta, *refs):
    pl.run_scoped(
        lambda load_sem, send_sem: kernel(load_sem, send_sem, n_xl, n_ta, *refs),
        pltpu.SemaphoreType.DMA((6 + len(BLOCKS),)),
        pltpu.SemaphoreType.DMA((len(OFFSETS),)),
    )


def solution(mesh):
    n_xl, n_ta = mesh.shape["xl"], mesh.shape["ta"]
    tables = filter_table(), halo_table(), rim_table()
    f32 = jnp.float32

    def shards(traces, steps):
        found = pl.pallas_call(
            functools.partial(scoped, n_xl, n_ta),
            name="stack_resample",
            out_shape=(
                jax.ShapeDtypeStruct((BROWS, BCOLS, OUT), f32),
                jax.ShapeDtypeStruct((2, BROWS, LANES), f32),
                jax.ShapeDtypeStruct((2, 8 * BROWS, SPAN), f32),
                jax.ShapeDtypeStruct((2, 2, BROWS, LANES), f32),
                jax.ShapeDtypeStruct((2, 2, 1, LANES), f32),
            ),
            in_specs=[pl.BlockSpec(memory_space=pltpu.HBM)] * 5,
            out_specs=(pl.BlockSpec(memory_space=pltpu.VMEM),) * 5,
            scratch_shapes=[
                pltpu.VMEM((ROWS, COLS, SPAN), f32),
                pltpu.VMEM((2, ROWS, 8, SPAN), f32),
                pltpu.VMEM((2, ROWS, COLS), jnp.int32),
                pltpu.VMEM((2, ROWS, SPAN), jnp.int32),
                pltpu.VMEM((3, SPAN, SPAN), jnp.bfloat16),
                pltpu.VMEM((2, 2, SPAN, SPAN), jnp.bfloat16),
                pltpu.VMEM((2, LANES, LANES), f32),
                pltpu.VMEM((BROWS, 3 * HALVES[0], SPAN), jnp.bfloat16),
                pltpu.VMEM((BROWS, 3 * HALVES[1], SPAN), jnp.bfloat16),
                pltpu.VMEM((BROWS + 2, HELD, OUT), f32),
                pltpu.VMEM((2, BROWS, 8, LANES), f32),
                pltpu.VMEM((2, 2 * BROWS, OUT), f32),
                pltpu.VMEM((2, 2, 2 * BROWS, LANES), f32),
                pltpu.VMEM((2, BROWS, 8, LANES), f32),
                pltpu.VMEM((2, 8, LANES), f32),
                pltpu.VMEM((HELD, OUT), f32),
                pltpu.VMEM((2, BROWS, OUT), f32),
                pltpu.VMEM((2, 1, OUT), f32),
                pltpu.VMEM((2, BROWS, 8, LANES), f32),
                pltpu.VMEM((2, 8, LANES), f32),
                pltpu.SemaphoreType.DMA((len(OFFSETS),)),
            ],
            compiler_params=pltpu.CompilerParams(
                collective_id=0, has_side_effects=True, vmem_limit_bytes=32 * 1024 * 1024
            ),
        )(*(pltpu.with_memory_space_constraint(a, pltpu.HBM) for a in (traces, steps, *map(jnp.asarray, tables))))
        return pl.pallas_call(
            lambda *refs: pl.run_scoped(
                lambda sems: finish(sems, *refs), pltpu.SemaphoreType.DMA((1 + BROWS,))
            ),
            name="finish",
            out_shape=jax.ShapeDtypeStruct((BROWS, BCOLS, OUT), f32),
            in_specs=[pl.BlockSpec(memory_space=pltpu.VMEM)] * 5,
            out_specs=pl.BlockSpec(memory_space=pltpu.HBM),
            scratch_shapes=[
                pltpu.VMEM((2, BROWS, BCOLS, LANES), f32),
            ],
            compiler_params=pltpu.CompilerParams(vmem_limit_bytes=16 * 1024 * 1024),
        )(*found)

    return jax.shard_map(
        shards,
        mesh=mesh,
        in_specs=(P("il", "xl", "ta"), P(None, "il", "xl")),
        out_specs=P("il", "xl", "ta"),
        check_vma=False,
    )
```

```python
import functools

import jax
import jax.numpy as jnp
import numpy as np
from jax import lax
from jax.experimental import pallas as pl
from jax.experimental.pallas import tpu as pltpu
from jax.sharding import PartitionSpec as P

TAPS = 16
P_SIZE = 3
Q = 2
REACH = TAPS // 2

LANES = 128
ROWS, COLS, SPAN = 16, 208, 256
BROWS, BCOLS, OUT = 8, 104, 384
HALVES = (64, 48)
STARTS = (0, 64)
HELD = 112
SPLIT = 56
FIRST_BIN, LAST_BIN = 0, 111
WINDOWS = ((0, 120), (104, 208))
GROUPS = tuple(range(0, 56, 8)) + tuple(range(64, 112, 8))

OFFSETS = tuple(
    (di, dx, dt) for di in (0, 1) for dx in (-1, 0, 1) for dt in (-1, 0, 1) if (di, dx, dt) != (0, 0, 0)
)


SIDES = ((-1, -1), (-1, 1), (1, -1), (1, 1), (0, -1), (0, 1), (-1, 0), (1, 0), (0, 0))
EARLY = SIDES[:4] + SIDES[6:8]
LATE = SIDES[4:6] + SIDES[8:]
BLOCKS = (range(0, 3), range(3, 8))


def filter_table():
    lane = np.arange(LANES)
    sample = np.stack(
        [
            np.where(lane < 112, lane, lane - 128),
            np.where(lane < 64, lane + 128, lane),
            np.where(lane < 16, lane + 256, lane + 128),
        ]
    )
    output = np.arange(OUT).reshape(3, LANES)
    x = (Q * output[:, None, :] - P_SIZE * sample[:, :, None]) / P_SIZE
    weights = np.where(np.abs(x) < REACH, np.sinc(x) * np.sinc(x / REACH), 0.0).astype(np.float32)
    high = weights.astype(jnp.bfloat16)
    low = (weights - high.astype(np.float32)).astype(jnp.bfloat16)
    top = np.concatenate([high, low], axis=2)
    bottom = np.concatenate([high, np.zeros_like(low)], axis=2)
    return np.concatenate([top, bottom], axis=1)


def halo_table():
    sample = np.arange(8)[:, None]
    weights = np.zeros((2, LANES, SPAN), np.float32)
    for end in (0, 1):
        n = sample - 8 if end else sample + SPAN
        x = (Q * (np.arange(16)[None, :] + (0 if end else OUT - 16)) - P_SIZE * n) / P_SIZE
        part = np.where(np.abs(x) < REACH, np.sinc(x) * np.sinc(x / REACH), 0.0)
        for r in range(len(GROUPS)):
            first = (8 * r + 120 * end) % LANES
            weights[end, first : first + 8, 16 * r : 16 * (r + 1)] = part
    high = weights.astype(jnp.bfloat16)
    low = (weights - high.astype(np.float32)).astype(jnp.bfloat16)
    return np.stack(
        [np.concatenate([high, high], axis=1), np.concatenate([low, np.zeros_like(low)], axis=1)], axis=1
    )


def rim_table():
    weights = np.zeros((2, LANES, LANES), np.float32)
    sample = np.arange(8)[:, None]
    for end in (0, 1):
        n = sample - 8 if end else sample + SPAN
        x = (Q * (np.arange(16)[None, :] + (0 if end else OUT - 16)) - P_SIZE * n) / P_SIZE
        part = np.where(np.abs(x) < REACH, np.sinc(x) * np.sinc(x / REACH), 0.0)
        first, place = (LANES - 8, 0) if end else (0, LANES - 16)
        weights[end, first : first + 8, place : place + 16] = part
    return weights


def in_group(r, end):
    start = (8 * r + (120 if end else 0)) % LANES
    lane = lax.broadcasted_iota(jnp.int32, (8, LANES), 1)
    return (lane >= start) & (lane < start + 8)


def parts_of(values):
    high = values.astype(jnp.bfloat16)
    low = (values - high.astype(jnp.float32)).astype(jnp.bfloat16)
    return high, low


def both(*conditions):
    held = [c for c in conditions if c is not None]
    return functools.reduce(jnp.logical_and, held) if held else None


def kernel(
    load_sem, send_sem, n_xl, n_ta, traces, steps, table, ends_table, rims_table, out, rim_scale, fixes, rf, rg,
    x, edges, sv, cbuf, tab, tab_ends, tab_rims, onehot0, onehot1, acc, scale_packed, rims, reach, packed, packed_rim,
    ra, rb, rc, rd, re, recv_sem,
):
    il, xl, ta = lax.axis_index("il"), lax.axis_index("xl"), lax.axis_index("ta")

    def there(step, index, size):
        return None if step == 0 else (index > 0 if step < 0 else index < size - 1)

    def device(offset):
        return {"il": 1 - il if offset[0] else il, "xl": xl + offset[1], "ta": ta + offset[2]}

    def for_neighbours(sides, action, sign=1):
        for dx, dt in sides:
            condition = both(there(sign * dx, xl, n_xl), there(sign * dt, ta, n_ta))

            def run(dx=dx, dt=dt):
                for di in (1, 0):
                    if (di, dx, dt) != (0, 0, 0):
                        action((di, dx, dt))

            if condition is None:
                run()
            else:
                pl.when(condition)(run)

    barrier = pltpu.get_barrier_semaphore()

    def greet(offset):
        pl.semaphore_signal(
            barrier, 1, device_id=device(offset), device_id_type=pl.DeviceIdType.MESH
        )

    for_neighbours(SIDES, greet)

    steps_copy = pltpu.make_async_copy(steps, sv, load_sem.at[0])
    steps_copy.start()
    edge_copies = []
    for side in (0, 1):
        columns = pl.ds((COLS - 8) * side, 8)
        edge_copies.append(pltpu.make_async_copy(traces.at[:, columns, :], edges.at[side], load_sem.at[1 + side]))
        edge_copies[-1].start()
    edge_copies.append(pltpu.make_async_copy(rims_table, tab_rims, load_sem.at[5 + len(BLOCKS)]))
    edge_copies[-1].start()
    loads = []
    for block in BLOCKS:
        rows = pl.ds(2 * block[0], 2 * len(block))
        loads.append(pltpu.make_async_copy(traces.at[rows], x.at[rows], load_sem.at[3 + len(loads)]))
        loads[-1].start()
    table_copies = [
        pltpu.make_async_copy(table, tab, load_sem.at[3 + len(BLOCKS)]),
        pltpu.make_async_copy(ends_table, tab_ends, load_sem.at[4 + len(BLOCKS)]),
    ]
    for copy in table_copies:
        copy.start()

    edge = (1 - il) * (BROWS + 1)
    target = BROWS - (BROWS - 1) * il

    own, far = pl.ds(0, BROWS), pl.ds(BROWS, 1)
    copies = {}
    for number, offset in enumerate(OFFSETS):
        di, dx, dt = offset
        side, end = (dx + 1) // 2, (dt + 1) // 2
        if dt == 0 and dx == 0:
            source, place = acc.at[edge], ra
        elif dt == 0:
            source, place = (rims.at[side, far], rc.at[side]) if di else (rims.at[side, own], rb.at[side])
        elif dx == 0:
            source, place = (packed_rim.at[end], re.at[end]) if di else (packed.at[end], rd.at[end])
        elif di:
            source, place = reach.at[end, side, far], rg.at[end, side]
        else:
            source, place = reach.at[end, side, own], rf.at[end, side]
        copies[offset] = pltpu.make_async_remote_copy(
            src_ref=source,
            dst_ref=place,
            send_sem=send_sem.at[number],
            recv_sem=recv_sem.at[number],
            device_id=device(offset),
            device_id_type=pl.DeviceIdType.MESH,
        )

    for dx in (-1, 1):
        side = (dx + 1) // 2

        @pl.when(jnp.logical_not(there(-dx, xl, n_xl)))
        def _(side=side):
            for place in (rb.at[side], rc.at[side], *(r.at[e, side] for r in (rf, rg) for e in (0, 1))):
                place[...] = jnp.zeros(place.shape, jnp.float32)

    for dt in (-1, 1):
        end = (dt + 1) // 2

        @pl.when(jnp.logical_not(there(-dt, ta, n_ta)))
        def _(end=end):
            for place in (rd.at[end], re.at[end], rf.at[end], rg.at[end]):
                place[...] = jnp.zeros(place.shape, jnp.float32)

    for copy in (steps_copy, *edge_copies):
        copy.wait()
    row_bin = lax.shift_right_logical(lax.broadcasted_iota(jnp.int32, (ROWS, COLS), 0), 1) + sv[0]
    inside = (row_bin >= 0) & (row_bin < BROWS)
    row_code = jnp.where(inside, row_bin, jnp.where(row_bin == edge - 1, BROWS, -1))
    def find_rims():
        slots = lax.broadcasted_iota(jnp.int32, (ROWS, 2 * BROWS), 1)
        ones = jnp.ones((2 * ROWS, LANES), jnp.float32)
        for side in (0, 1):
            code = jnp.where(sv[1] == 2 * side - 1, row_code, -1)
            chosen, values = [], []
            for j in (0, 1):
                column = (COLS - 2) * side + j
                chosen.append(jnp.where(slots == code[:, column : column + 1], 1.0, 0.0))
                values.append(edges[side, :, 6 * side + j, :])
            rims[side] = lax.dot_general(
                jnp.concatenate(chosen, axis=0),
                jnp.concatenate([jnp.concatenate(values, axis=0), ones], axis=1),
                (((0,), (0,)), ((), ())),
                precision=lax.Precision.HIGHEST,
                preferred_element_type=jnp.float32,
            )
        for end in (0, 1):
            tiles = [rims[side, :, LANES * end : LANES * (end + 1)] for side in (0, 1)]
            product = jnp.dot(
                jnp.concatenate(tiles, axis=0),
                tab_rims[end],
                precision=lax.Precision.HIGHEST,
                preferred_element_type=jnp.float32,
            )
            for side in (0, 1):
                reach[end, side] = product[2 * BROWS * side : 2 * BROWS * (side + 1)]

    find_rims()

    wide = lax.broadcasted_iota(jnp.int32, (ROWS, SPAN), 1)
    bin_col = lax.shift_right_logical(lax.broadcasted_iota(jnp.int32, (ROWS, COLS), 1), 1) + sv[1]
    cbuf[...] = jnp.full(cbuf.shape, -1, jnp.int32)
    cbuf[0, :, 0:COLS] = jnp.where(
        (bin_col >= 0) & (bin_col < SPLIT), (sv[0] + 1) * HALVES[0] + bin_col, -1
    )
    cbuf[1, :, 0:COLS] = jnp.where(
        (bin_col >= SPLIT) & (bin_col < BCOLS), (sv[0] + 1) * HALVES[1] + bin_col - SPLIT, -1
    )
    first, second = cbuf[0], cbuf[1]
    codes = (
        (
            jnp.where(wide < 120, first, -1),
            jnp.where((wide >= 120) & (wide < 240), pltpu.roll(first, 120, 1), -1),
        ),
        (
            jnp.where(wide < 104, pltpu.roll(second, SPAN - 104, 1), -1),
            jnp.where((wide >= 104) & (wide < 208), second, -1),
        ),
    )
    onehot = (onehot0, onehot1)
    for h, size in enumerate(HALVES):
        places = lax.broadcasted_iota(jnp.int32, (3 * size, SPAN), 0)
        even, odd = codes[h]
        for k in range(BROWS):
            code = jnp.maximum(even[2 * k : 2 * k + 1], odd[2 * k + 1 : 2 * k + 2])
            onehot[h][k] = jnp.where(places == code, 1.0, 0.0).astype(jnp.bfloat16)

    for b in range(BROWS + 2):
        for h, size in enumerate(HALVES):
            rows = [onehot[h][k, size * (b - k) : size * (b - k + 1), :] for k in range(BROWS) if 0 <= b - k < 3]
            total = functools.reduce(jnp.add, rows)
            total = (total[:, :LANES] + total[:, LANES:]).astype(jnp.float32)
            acc[b, STARTS[h] : STARTS[h] + size, SPAN:OUT] = jnp.broadcast_to(
                jnp.sum(total, axis=1, keepdims=True), (size, LANES)
            )

    lane = lax.broadcasted_iota(jnp.int32, (8, LANES), 1)
    def pack(b, end):
        tile = pl.ds(LANES * end, LANES)
        total = acc[b, 0:8, tile]
        for r in range(1, len(GROUPS)):
            turned = pltpu.roll(acc[b, GROUPS[r] : GROUPS[r] + 8, tile], 8 * r, 1)
            total = jnp.where(in_group(r, end), turned, total)
        return total

    def send(offset):
        copies[offset].start()

    distant = (lax.rem(ta, 4) == 0) | (ta == n_ta // 2 - 1)

    def meet():
        beside_xl = 1 + (xl > 0).astype(jnp.int32) + (xl < n_xl - 1).astype(jnp.int32)
        beside_ta = 1 + (ta > 0).astype(jnp.int32) + (ta < n_ta - 1).astype(jnp.int32)
        pl.semaphore_wait(barrier, 2 * beside_xl * beside_ta - 1)

    for block, load in zip(BLOCKS, loads):
        load.wait()
        for k in block:
            for h, size in enumerate(HALVES):
                start, stop = WINDOWS[h]
                pieces = [x[2 * k, start:stop, :], x[2 * k + 1, start:stop, :]]
                pieces.append(jnp.zeros((SPAN - 2 * (stop - start), SPAN), jnp.float32))
                high, low = parts_of(jnp.concatenate(pieces, axis=0))
                chosen = onehot[h][k]
                result = jnp.dot(chosen, high, preferred_element_type=jnp.float32)
                result = result + jnp.dot(chosen, low, preferred_element_type=jnp.float32)
                for q in range(3):
                    b = k + q
                    where = (b, pl.ds(STARTS[h], size), pl.ds(0, SPAN))
                    part = result[size * q : size * (q + 1)]
                    acc[where] = part if k == max(b - 2, 0) else acc[where] + part
            if k > 0:
                for end in (0, 1):
                    packed[end, k - 1] = pack(k, end)
        if block is BLOCKS[0]:

            @pl.when(jnp.logical_not(distant))
            def _():
                meet()
                for_neighbours(EARLY, send)

    for end in (0, 1):
        packed[end, BROWS - 1] = pack(BROWS, end)
        packed_rim[end] = pack(edge, end)

    @pl.when(distant)
    def _():
        meet()
        for_neighbours(EARLY, send)

    for_neighbours(LATE, send)

    for_neighbours(SIDES[6:], lambda offset: copies[offset].wait_recv(), -1)
    acc[target] = acc[target] + ra[...]
    for row, side in ((FIRST_BIN, 1), (LAST_BIN, 0)):
        acc[target, row : row + 1, :] = acc[target, row : row + 1, :] + rc[side]
        for b in range(BROWS):
            acc[b + 1, row : row + 1, :] = acc[b + 1, row : row + 1, :] + rb[side, b : b + 1, :]

    for copy in table_copies:
        copy.wait()

    def bins(b, tile):
        lanes = pl.ds(LANES * tile, LANES)
        return [acc[b, 0:SPLIT, lanes], acc[b, STARTS[1] : HELD, lanes]]

    def pair(p, tile):
        return jnp.concatenate(bins(2 * p + 1, tile) + bins(2 * p + 2, tile), axis=0)

    across = lax.broadcasted_iota(jnp.int32, (2 * BCOLS, LANES), 1)

    def resample(p, third, window):
        high, low = parts_of(window)
        result = jnp.dot(
            jnp.concatenate([high, low], axis=1), tab[third], preferred_element_type=jnp.float32
        )
        result = result[:, :LANES] + result[:, LANES:]
        lanes = pl.ds(LANES * third, LANES)
        out[2 * p, :, lanes] = result[:BCOLS]
        out[2 * p + 1, :, lanes] = result[BCOLS:]

    for p in range(BROWS // 2):
        factor = 1.0 / jnp.maximum(pair(p, 2), 1.0)
        low, high = pair(p, 0), pair(p, 1)
        resample(p, 1, jnp.where(across < 64, high, low) * factor)
        resample(p, 0, jnp.where(across < 112, low, 0.0) * factor)
        resample(p, 2, jnp.where(across < 16, 0.0, high) * factor)
        for b in (0, 1):
            for n, c in enumerate((0, BCOLS - 1)):
                row = BCOLS * b + c
                rim_scale[n, 2 * p + b : 2 * p + b + 1, :] = factor[row : row + 1]
            for end in (0, 1):
                total = jnp.zeros((8, LANES), jnp.float32)
                for r in range(len(GROUPS)):
                    row = BCOLS * b + 8 * r
                    total = jnp.where(in_group(r, end), factor[row : row + 8], total)
                scale_packed[end, 2 * p + b] = total
    for_neighbours(SIDES, lambda offset: copies[offset].wait_send())

    for_neighbours(SIDES[4:6], lambda offset: copies[offset].wait_recv(), -1)
    for end in (0, 1):
        rows = []
        for b in range(BROWS):
            tile = rd[end, b]
            if b in (0, BROWS - 1):
                tile = tile + jnp.where(target == b + 1, re[end], 0.0)
            rows.append(tile * scale_packed[end, b])
        fixes[end] = halo_product(jnp.concatenate(rows, axis=0), tab_ends, end)
    for_neighbours(SIDES[:4], lambda offset: copies[offset].wait_recv(), -1)


def halo_product(packed, tab_ends, end):
    high, low = parts_of(packed)
    halves = jnp.concatenate([high, low], axis=1)
    result = jnp.dot(halves, tab_ends[end, 0], preferred_element_type=jnp.float32)
    return result + jnp.dot(halves, tab_ends[end, 1], preferred_element_type=jnp.float32)


def finish(sems, own, rim_scale, fixes, rf, rg, out, ends):
    middle = pl.ds(LANES, LANES)
    copies = [pltpu.make_async_copy(own.at[:, :, middle], out.at[:, :, middle], sems.at[0])]
    copies[0].start()
    lane = lax.broadcasted_iota(jnp.int32, (8, LANES), 1)
    sublane = lax.broadcasted_iota(jnp.int32, (8, LANES), 0)
    target = BROWS - (BROWS - 1) * lax.axis_index("il")

    last = len(GROUPS) - 1

    def rims(end, n):
        far = jnp.where(sublane == target - 1, jnp.broadcast_to(rg[end, 1 - n], (8, LANES)), 0.0)
        return (rf[end, 1 - n] + far) * rim_scale[n]

    added = [[rims(end, n) for n in (0, 1)] for end in (0, 1)]

    def part_of(b, r, end):
        tile = slice(LANES * (r // 8), LANES * (r // 8 + 1))
        part = fixes[end, 8 * b : 8 * (b + 1), tile]
        turn = ((0 if end else 112) - 16 * (r % 8)) % LANES
        part = pltpu.roll(part, turn, 1) if turn else part
        part = jnp.where(lane < 16 if end else lane >= 112, part, 0.0)
        if r in (0, last):
            n = min(r, 1)
            part = part + jnp.where(sublane == 7 * n, added[end][n][b : b + 1], 0.0)
        return part

    for p in range(BROWS // 2):
        for b in (2 * p, 2 * p + 1):
            for r in range(len(GROUPS)):
                rows = pl.ds(8 * r, 8)
                ends[1, b, rows, :] = own[b, rows, 0:LANES] + part_of(b, r, 1)
                ends[0, b, rows, :] = own[b, rows, 2 * LANES : OUT] + part_of(b, r, 0)
        for end in (0, 1):
            bs = pl.ds(2 * p, 2)
            lanes = pl.ds(0 if end else 2 * LANES, LANES)
            copies.append(pltpu.make_async_copy(ends.at[end, bs], out.at[bs, :, lanes], sems.at[len(copies)]))
            copies[-1].start()
    for copy in copies:
        copy.wait()


def scoped(n_xl, n_ta, *refs):
    pl.run_scoped(
        lambda load_sem, send_sem: kernel(load_sem, send_sem, n_xl, n_ta, *refs),
        pltpu.SemaphoreType.DMA((6 + len(BLOCKS),)),
        pltpu.SemaphoreType.DMA((len(OFFSETS),)),
    )


def solution(mesh):
    n_xl, n_ta = mesh.shape["xl"], mesh.shape["ta"]
    tables = filter_table(), halo_table(), rim_table()
    f32 = jnp.float32

    def shards(traces, steps):
        found = pl.pallas_call(
            functools.partial(scoped, n_xl, n_ta),
            name="stack_resample",
            out_shape=(
                jax.ShapeDtypeStruct((BROWS, BCOLS, OUT), f32),
                jax.ShapeDtypeStruct((2, BROWS, LANES), f32),
                jax.ShapeDtypeStruct((2, 8 * BROWS, SPAN), f32),
                jax.ShapeDtypeStruct((2, 2, BROWS, LANES), f32),
                jax.ShapeDtypeStruct((2, 2, 1, LANES), f32),
            ),
            in_specs=[pl.BlockSpec(memory_space=pltpu.HBM)] * 5,
            out_specs=(pl.BlockSpec(memory_space=pltpu.VMEM),) * 5,
            scratch_shapes=[
                pltpu.VMEM((ROWS, COLS, SPAN), f32),
                pltpu.VMEM((2, ROWS, 8, SPAN), f32),
                pltpu.VMEM((2, ROWS, COLS), jnp.int32),
                pltpu.VMEM((2, ROWS, SPAN), jnp.int32),
                pltpu.VMEM((3, SPAN, SPAN), jnp.bfloat16),
                pltpu.VMEM((2, 2, SPAN, SPAN), jnp.bfloat16),
                pltpu.VMEM((2, LANES, LANES), f32),
                pltpu.VMEM((BROWS, 3 * HALVES[0], SPAN), jnp.bfloat16),
                pltpu.VMEM((BROWS, 3 * HALVES[1], SPAN), jnp.bfloat16),
                pltpu.VMEM((BROWS + 2, HELD, OUT), f32),
                pltpu.VMEM((2, BROWS, 8, LANES), f32),
                pltpu.VMEM((2, 2 * BROWS, OUT), f32),
                pltpu.VMEM((2, 2, 2 * BROWS, LANES), f32),
                pltpu.VMEM((2, BROWS, 8, LANES), f32),
                pltpu.VMEM((2, 8, LANES), f32),
                pltpu.VMEM((HELD, OUT), f32),
                pltpu.VMEM((2, BROWS, OUT), f32),
                pltpu.VMEM((2, 1, OUT), f32),
                pltpu.VMEM((2, BROWS, 8, LANES), f32),
                pltpu.VMEM((2, 8, LANES), f32),
                pltpu.SemaphoreType.DMA((len(OFFSETS),)),
            ],
            compiler_params=pltpu.CompilerParams(
                collective_id=0, has_side_effects=True, vmem_limit_bytes=32 * 1024 * 1024
            ),
        )(*(pltpu.with_memory_space_constraint(a, pltpu.HBM) for a in (traces, steps, *map(jnp.asarray, tables))))
        return pl.pallas_call(
            lambda *refs: pl.run_scoped(
                lambda sems: finish(sems, *refs), pltpu.SemaphoreType.DMA((1 + BROWS,))
            ),
            name="finish",
            out_shape=jax.ShapeDtypeStruct((BROWS, BCOLS, OUT), f32),
            in_specs=[pl.BlockSpec(memory_space=pltpu.VMEM)] * 5,
            out_specs=pl.BlockSpec(memory_space=pltpu.HBM),
            scratch_shapes=[
                pltpu.VMEM((2, BROWS, BCOLS, LANES), f32),
            ],
            compiler_params=pltpu.CompilerParams(vmem_limit_bytes=16 * 1024 * 1024),
        )(*found)

    return jax.shard_map(
        shards,
        mesh=mesh,
        in_specs=(P("il", "xl", "ta"), P(None, "il", "xl")),
        out_specs=P("il", "xl", "ta"),
        check_vma=False,
    )
```
